32 devices in a mesh: dp: 4 (over x, y), tp: 8 (over z, core).
Axes of the slice: x: 2, y: 2, z: 4, core: 2. Of those that a mesh axis runs over, the one named last changes fastest.
Arguments:
- x: bfloat16 [15360, 2304], P(('dp', 'tp')), parts along dimension 0
- dy: bfloat16 [15360, 2304], P(('dp', 'tp')), parts along dimension 0
- gate: bfloat16 [15360, 9216], P('dp', 'tp'), parts along dimension 0
- up: bfloat16 [15360, 9216], P('dp', 'tp'), parts along dimension 0
- w_gate: bfloat16 [2304, 9216], P(None, 'tp')
- w_up: bfloat16 [2304, 9216], P(None, 'tp')
- w_down: bfloat16 [9216, 2304], P('tp')
Outputs:
- output 1: bfloat16 [15360, 2304], P(('dp', 'tp')), parts along dimension 0
- output 2: bfloat16 [9216, 9216], P('dp', 'tp'), parts along dimension 0
- output 3: bfloat16 [9216, 9216], P('dp', 'tp'), parts along dimension 0
- output 4: bfloat16 [36864, 2304], P(('dp', 'tp')), parts along dimension 0
There are 4 independent parts. The reference program is written for one: setup_inputs(seed, part) draws one part's arguments, and reference() takes and returns one part's arrays. A program takes and returns all parts, laid end to end along the dimension named above; an argument that names none is the same for every part.
All inputs are finite; a program needn't handle non-finite values.
Results may differ from the reference program's by a relative error of at most 0.012.
Values are sent between devices in bfloat16 or wider.
A program may use at most 2 GiB of HBM per device.

```python
import jax
import jax.numpy as jnp

ROWS = 3840
D = 2304
FF = 9216


def act(gate, up):
    return jax.nn.gelu(gate) * up


def setup_inputs(seed: int = 0, part: int = 0) -> dict:
    kx, ky, ka, kb, kg, ku, kd = jax.random.split(jax.random.key(seed), 7)
    kx, ky, ka, kb = (jax.random.fold_in(k, part) for k in (kx, ky, ka, kb))
    drawn = {
        "x": jax.random.normal(kx, (ROWS, D), jnp.float32),
        "dy": jax.random.normal(ky, (ROWS, D), jnp.float32),
        "gate": jax.random.normal(ka, (ROWS, FF), jnp.float32),
        "up": jax.random.normal(kb, (ROWS, FF), jnp.float32),
        "w_gate": jax.random.normal(kg, (D, FF), jnp.float32) * D**-0.5,
        "w_up": jax.random.normal(ku, (D, FF), jnp.float32) * D**-0.5,
        "w_down": jax.random.normal(kd, (FF, D), jnp.float32) * FF**-0.5,
    }
    return {k: v.astype(jnp.bfloat16) for k, v in drawn.items()}


def reference(x, dy, gate, up, w_gate, w_up, w_down):
    hidden, back = jax.vjp(act, gate.astype(jnp.float32), up.astype(jnp.float32))
    d_hidden = jnp.dot(dy, w_down.T, preferred_element_type=jnp.float32)
    d_gate, d_up = (g.astype(jnp.bfloat16) for g in back(d_hidden))
    dx = jnp.dot(d_gate, w_gate.T, preferred_element_type=jnp.float32) + jnp.dot(d_up, w_up.T, preferred_element_type=jnp.float32)
    dw_gate = jnp.dot(x.T, d_gate, preferred_element_type=jnp.float32)
    dw_up = jnp.dot(x.T, d_up, preferred_element_type=jnp.float32)
    dw_down = jnp.dot(hidden.astype(jnp.bfloat16).T, dy, preferred_element_type=jnp.float32)
    return tuple(g.astype(jnp.bfloat16) for g in (dx, dw_gate, dw_up, dw_down))
```

```python
import functools

import jax
import jax.numpy as jnp
from jax import lax
from jax.experimental import pallas as pl
from jax.experimental.pallas import tpu as pltpu
from jax.sharding import PartitionSpec as P

MESH = pl.DeviceIdType.MESH
F32, BF16 = jnp.float32, jnp.bfloat16
H = 3


def act(gate, up):
    return jax.nn.gelu(gate) * up


def dot(a, b, ca, cb):
    return lax.dot_general(a, b, (((ca,), (cb,)), ((), ())), preferred_element_type=F32)


def tile_of(n, cap):
    return max(t for t in range(128, min(n, cap) + 1, 128) if n % t == 0)


MID_M = {0: 0, 1: 1, -1: 2, 2: 3}


def kernel(x_ref, dy_ref, gate_ref, up_ref, wg_ref, wu_ref, wd_ref,
           dx_ref, dwg_ref, dwu_ref, dwd_ref,
           dyg, xg, dgs, dus, pown, pin, tst, ru, rv, rw, rso,
           xv, gv, uv, pc, tc, rc, sc, oc,
           sF, sE, rF, rE, sP, rP, sT, rT, sU, rU, sV, rV, sW, rW, lsem):
    S, D = x_ref.shape
    F = gate_ref.shape[1]
    C = S // H
    tp = lax.axis_index("tp")
    z, c = tp // 2, tp % 2
    way = jnp.where(z < 2, 1, -1)
    is_end = (z == 0) | (z == 3)
    is_mid = (z == 1) | (z == 2)

    def chip(k):
        return z + way * k

    def dev(k):
        return {"tp": 2 * chip(k) + c}

    partner = {"tp": 2 * z + 1 - c}
    rows = lambda h: pl.ds(h * C, C)
    given, gathered = (dy_ref, x_ref), (dyg, xg)

    def rcopy(src, dst, ssem, rsem, to):
        return pltpu.make_async_remote_copy(
            src_ref=src, dst_ref=dst, send_sem=ssem, recv_sem=rsem, device_id=to, device_id_type=MESH)

    def local(*copies):
        made = [pltpu.make_async_copy(s, d, lsem.at[i]) for i, (s, d) in enumerate(copies)]
        for cp in made:
            cp.start()
        for cp in made:
            cp.wait()

    def piece(a, k, h):
        return gathered[a].at[2 * chip(k) + c, rows(h)]

    def source(a, k, h):
        return given[a].at[rows(h)] if k == 0 else piece(a, k, h)

    def end_to_f(a, h):
        return rcopy(source(a, 0, h), piece(a, 0, h), sF.at[a, 0, h], rE.at[a, h], dev(1))

    def mid_to_f(a, k, h):
        j = 0 if k == 0 else 1
        return rcopy(source(a, k, h), piece(a, k, h), sF.at[a, j, h], rF.at[a, j, h], dev(1))

    def mid_to_e(a, k, h):
        return rcopy(source(a, k, h), piece(a, k, h), sE.at[a, k, h], rF.at[a, k, h], dev(-1))

    def to_partner(a, k, m):
        src = given[a] if k == 0 else gathered[a].at[2 * chip(k) + c]
        return rcopy(src, gathered[a].at[2 * chip(k) + c], sP.at[a, m], rP.at[a, m], partner)

    def wait_f(a, k, h):
        rcopy(piece(a, k, h), piece(a, k, h), sF.at[a, 0, h], rF.at[a, k - 1, h], partner).wait_recv()

    def wait_e(a, h):
        rcopy(piece(a, -1, h), piece(a, -1, h), sF.at[a, 0, h], rE.at[a, h], partner).wait_recv()

    def term(m):
        return rcopy(tst.at[m], pin.at[m], sT.at[m], rT.at[m], partner)

    def u_copy(j, h):
        return rcopy(rso.at[j, rows(h)], ru.at[j, rows(h)], sU.at[j, h], rU.at[j, h], dev(1))

    def v_copy(j, h):
        return rcopy(rso.at[j, rows(h)], rv.at[j, rows(h)], sV.at[j, h], rV.at[j, h], dev(1))

    def w_copy(h):
        return rcopy(rso.at[2, rows(h)], rw.at[rows(h)], sW.at[h], rW.at[h], dev(-1))

    def combine(m, h, received, out):
        bufs = [pc, tc, rc, sc]
        srcs = [pown.at[m, rows(h)], pin.at[m, rows(h)], *received]
        local(*zip(srcs, bufs))
        step = 16

        @pl.loop(0, C // step)
        def _(i):
            r = pl.ds(pl.multiple_of(i * step, step), step)
            total = pc[r, :] + tc[r, :].astype(F32)
            for b in bufs[2:len(srcs)]:
                total += b[r, :].astype(F32)
            oc[r, :] = total.astype(BF16)

        local((oc, out))

    barrier = pltpu.get_barrier_semaphore()
    pl.semaphore_signal(barrier, inc=1, device_id=partner, device_id_type=MESH)
    pl.semaphore_signal(barrier, inc=1, device_id=dev(1), device_id_type=MESH)

    @pl.when(is_mid)
    def _():
        pl.semaphore_signal(barrier, inc=1, device_id=dev(-1), device_id_type=MESH)
        pl.semaphore_wait(barrier, 3)

    @pl.when(is_end)
    def _():
        pl.semaphore_wait(barrier, 2)

    @pl.when(is_mid)
    def _():
        for h in range(H):
            mid_to_e(0, 0, h).start()
            mid_to_f(0, 0, h).start()

    @pl.when(is_end)
    def _():
        for h in range(H):
            end_to_f(0, h).start()
        for h in range(H):
            end_to_f(1, h).start()

    for a in range(2):
        to_partner(a, 0, 0).start()

    def k_of(m):
        mid = jnp.where(m == 2, -1, jnp.where(m == 3, 2, m))
        return jnp.where(is_end, m, mid)

    def load_shard(a, m, p):
        t = 2 * (z + way * k_of(m)) + jnp.where(p == 0, c, 1 - c)

        @pl.when(p == 1)
        def _():
            rcopy(gathered[a].at[t], gathered[a].at[t], sP.at[a, m], rP.at[a, m], partner).wait_recv()

        @pl.when((m == 0) & (p == 0))
        def _():
            pltpu.make_async_copy(given[a], xv, lsem.at[2]).start()

        @pl.when((m > 0) | (p > 0))
        def _():
            pltpu.make_async_copy(gathered[a].at[t], xv, lsem.at[2]).start()

        return t

    def phase1(wd, wg, wu, accd, hid, dgv, duv, dxf, dxb, stage):
        local((wd_ref, wd), (wg_ref, wg))
        local((wu_ref, wu))
        accd[...] = jnp.zeros_like(accd)

        def unit(m, p):
            t = load_shard(0, m, p)
            local((gate_ref.at[pl.ds(t * S, S)], gv), (up_ref.at[pl.ds(t * S, S)], uv))
            pltpu.make_async_copy(given[0], xv, lsem.at[2]).wait()
            tn = min(F, 256)

            @pl.loop(0, pl.cdiv(F, tn))
            def _(n):
                s = pl.ds(pl.multiple_of(jnp.minimum(n * tn, F - tn), 128), tn)
                d_hidden = dot(xv[...], wd[s, :], 1, 1)
                hidden, back = jax.vjp(act, gv[:, s].astype(F32), uv[:, s].astype(F32))
                d_gate, d_up = back(d_hidden)
                hid[:, s] = hidden.astype(BF16)
                dgv[:, s] = d_gate.astype(BF16)
                duv[:, s] = d_up.astype(BF16)

            keep = [pltpu.make_async_copy(v, o.at[2 * m + p], lsem.at[i])
                    for i, (v, o) in enumerate(((dgv, dgs), (duv, dus)))]
            for cp in keep:
                cp.start()
            tn2 = tile_of(D, 256)

            @pl.loop(0, D // tn2)
            def _(n):
                s = pl.ds(pl.multiple_of(n * tn2, tn2), tn2)
                part = dot(dgv[...], wg[s, :], 1, 1) + dot(duv[...], wu[s, :], 1, 1)
                dxf[:, s] = part
                dxb[:, s] = part.astype(BF16)

            for cp in keep:
                cp.wait()

            @pl.when(p == 0)
            def _():
                local((dxf, pown.at[m]))

            @pl.when(p == 1)
            def _():
                local((dxb, tst.at[m]))
                term(m).start()

            tn3 = tile_of(D, 768)

            @pl.loop(0, D // tn3)
            def _(n):
                s = pl.ds(pl.multiple_of(n * tn3, tn3), tn3)
                accd[:, s] += dot(hid[...], xv[:, s], 0, 0)

        def wait_term(m):
            term(m).wait_recv()

        def send_u(j):
            wait_term(j + 1)
            for h in range(H):
                combine(j + 1, h, [], rso.at[j, rows(h)])
                u_copy(j, h).start()

        @pl.loop(0, 4)
        def _(m):
            @pl.loop(0, 2)
            def _(p):
                unit(m, p)

            @pl.when((m == 0) & is_end)
            def _():
                for h in range(H):
                    wait_f(0, 1, h)
                to_partner(0, 1, 1).start()

            @pl.when((m == 0) & is_mid)
            def _():
                for h in range(H):
                    wait_f(0, 1, h)
                    mid_to_e(0, 1, h).start()
                    wait_e(0, h)
                    mid_to_f(0, -1, h).start()
                to_partner(0, 1, 1).start()
                to_partner(0, -1, 2).start()
                for h in range(H):
                    mid_to_f(1, 0, h).start()

            @pl.when((m == 1) & is_end)
            def _():
                send_u(0)
                for h in range(H):
                    wait_f(0, 2, h)
                to_partner(0, 2, 2).start()

            @pl.when((m == 1) & is_mid)
            def _():
                for h in range(H):
                    wait_f(0, 2, h)
                    mid_to_e(0, 2, h).start()
                to_partner(0, 2, 3).start()
                for h in range(H):
                    mid_to_e(1, 0, h).start()
                for h in range(H):
                    wait_e(1, h)
                    mid_to_f(1, -1, h).start()
                to_partner(1, -1, 2).start()

            @pl.when((m == 2) & is_end)
            def _():
                send_u(1)
                for h in range(H):
                    wait_f(0, 3, h)
                to_partner(0, 3, 3).start()

            @pl.when((m == 2) & is_mid)
            def _():
                for h in range(H):
                    wait_f(1, 1, h)
                    mid_to_e(1, 1, h).start()
                to_partner(1, 1, 1).start()

            @pl.when((m == 3) & is_end)
            def _():
                send_u(2)

        flush(accd, dwd_ref, stage)

    def flush(acc, out, stage):
        n = stage.shape[0]

        @pl.loop(0, acc.shape[0] // n)
        def _(i):
            r = pl.ds(pl.multiple_of(i * n, n), n)
            stage[...] = acc[r, :].astype(BF16)
            local((stage, out.at[r]))

    def send_v(j):
        m = MID_M[j + 1]
        term(m).wait_recv()
        for h in range(H):
            rcopy(ru.at[j + 1, rows(h)], ru.at[j + 1, rows(h)], sU.at[j + 1, h], rU.at[j + 1, h], partner).wait_recv()
            combine(m, h, [ru.at[j + 1, rows(h)]], rso.at[j, rows(h)])
            v_copy(j, h).start()

    def send_w():
        m = MID_M[-1]
        term(m).wait_recv()
        for h in range(H):
            rcopy(rv.at[1, rows(h)], rv.at[1, rows(h)], sV.at[1, h], rV.at[1, h], partner).wait_recv()
            combine(m, h, [rv.at[1, rows(h)]], rso.at[2, rows(h)])
            w_copy(h).start()

    def phase2(accg, accu, stage):
        accg[...] = jnp.zeros_like(accg)
        accu[...] = jnp.zeros_like(accu)

        def unit(m, p):
            load_shard(1, m, p)
            local((dgs.at[2 * m + p], gv), (dus.at[2 * m + p], uv))
            pltpu.make_async_copy(given[1], xv, lsem.at[2]).wait()
            tm = tile_of(D, 768)

            @pl.loop(0, D // tm)
            def _(n):
                s = pl.ds(pl.multiple_of(n * tm, tm), tm)
                accg[s, :] += dot(xv[:, s], gv[...], 0, 0)
                accu[s, :] += dot(xv[:, s], uv[...], 0, 0)

        @pl.loop(0, 4)
        def _(m):
            @pl.when((m == 0) & is_mid)
            def _():
                send_v(0)

            @pl.when((m == 1) & is_mid)
            def _():
                for h in range(H):
                    wait_f(1, 2, h)
                    mid_to_e(1, 2, h).start()
                to_partner(1, 2, 3).start()

            @pl.when((m == 3) & is_mid)
            def _():
                send_v(1)

            for i in range(1, 4):
                @pl.when((m == i) & is_end)
                def _(i=i):
                    for h in range(H):
                        wait_f(1, i, h)
                    to_partner(1, i, i).start()

            @pl.loop(0, 2)
            def _(p):
                unit(m, p)

        @pl.when(is_mid)
        def _():
            send_w()

        flush(accg, dwg_ref, stage)
        flush(accu, dwu_ref, stage)

    wbuf = lambda r: pltpu.VMEM(r.shape, r.dtype)
    pl.run_scoped(
        phase1, wbuf(wd_ref), wbuf(wg_ref), wbuf(wu_ref), pltpu.VMEM((F, D), F32),
        pltpu.VMEM((S, F), BF16), pltpu.VMEM((S, F), BF16), pltpu.VMEM((S, F), BF16),
        pltpu.VMEM((S, D), F32), pltpu.VMEM((S, D), BF16), pltpu.VMEM((tile_of(F, 384), D), BF16))
    pl.run_scoped(
        phase2, pltpu.VMEM((D, F), F32), pltpu.VMEM((D, F), F32), pltpu.VMEM((tile_of(D, 768), F), BF16))

    term(0).wait_recv()

    @pl.when(is_mid)
    def _():
        for h in range(H):
            rcopy(ru.at[0, rows(h)], ru.at[0, rows(h)], sU.at[0, h], rU.at[0, h], partner).wait_recv()
            rcopy(rv.at[0, rows(h)], rv.at[0, rows(h)], sV.at[0, h], rV.at[0, h], partner).wait_recv()
            combine(0, h, [ru.at[0, rows(h)], rv.at[0, rows(h)]], dx_ref.at[rows(h)])

    @pl.when(is_end)
    def _():
        for h in range(H):
            rcopy(rw.at[rows(h)], rw.at[rows(h)], sW.at[h], rW.at[h], partner).wait_recv()
            combine(0, h, [rw.at[rows(h)]], dx_ref.at[rows(h)])

    for m in range(4):
        term(m).wait_send()

    @pl.when(is_end)
    def _():
        for a in range(2):
            for h in range(H):
                end_to_f(a, h).wait_send()
            for k in range(4):
                to_partner(a, k, k).wait_send()
        for j in range(3):
            for h in range(H):
                u_copy(j, h).wait_send()

    @pl.when(is_mid)
    def _():
        for a in range(2):
            for h in range(H):
                for k in (0, 1, 2):
                    mid_to_e(a, k, h).wait_send()
                for k in (0, -1):
                    mid_to_f(a, k, h).wait_send()
            for k, m in MID_M.items():
                to_partner(a, k, m).wait_send()
        for h in range(H):
            for j in range(2):
                v_copy(j, h).wait_send()
            w_copy(h).wait_send()


def solution(mesh):
    def step(x, dy, gate, up, w_gate, w_up, w_down):
        (S, D), F = x.shape, gate.shape[1]
        C = S // H
        shape = jax.ShapeDtypeStruct
        any_ = pl.BlockSpec(memory_space=pl.ANY)
        outs = [
            shape((S, D), BF16), shape((D, F), BF16), shape((D, F), BF16), shape((F, D), BF16),
            shape((8, S, D), BF16), shape((8, S, D), BF16),
            shape((8, S, F), BF16), shape((8, S, F), BF16),
            shape((4, S, D), F32), shape((4, S, D), BF16), shape((4, S, D), BF16),
            shape((3, S, D), BF16), shape((2, S, D), BF16), shape((S, D), BF16), shape((3, S, D), BF16),
        ]
        dma = pltpu.SemaphoreType.DMA
        out = pl.pallas_call(
            kernel,
            out_shape=outs,
            in_specs=[any_] * 7,
            out_specs=[any_] * len(outs),
            scratch_shapes=[
                pltpu.VMEM((S, D), BF16), pltpu.VMEM((S, F), BF16), pltpu.VMEM((S, F), BF16),
                pltpu.VMEM((C, D), F32), pltpu.VMEM((C, D), BF16), pltpu.VMEM((C, D), BF16),
                pltpu.VMEM((C, D), BF16), pltpu.VMEM((C, D), BF16),
                dma((2, 2, H)), dma((2, 3, H)), dma((2, 3, H)), dma((2, H)),
                dma((2, 4)), dma((2, 4)), dma((4,)), dma((4,)),
                dma((3, H)), dma((3, H)), dma((2, H)), dma((2, H)), dma((H,)), dma((H,)),
                dma((4,)),
            ],
            compiler_params=pltpu.CompilerParams(
                collective_id=0, has_side_effects=True, vmem_limit_bytes=60 * 2**20),
            name="mlp_backward",
        )(x, dy, gate, up, w_gate, w_up, w_down)
        return tuple(out[:4])

    both = P(("dp", "tp"), None)
    cols = P("dp", "tp")
    return jax.shard_map(
        step, mesh=mesh,
        in_specs=(both, both, cols, cols, P(None, "tp"), P(None, "tp"), P("tp", None)),
        out_specs=(both, cols, cols, both), check_vma=False)
```

```python
import functools

import jax
import jax.numpy as jnp
from jax import lax
from jax.experimental import pallas as pl
from jax.experimental.pallas import tpu as pltpu
from jax.sharding import PartitionSpec as P

MESH = pl.DeviceIdType.MESH
F32, BF16 = jnp.float32, jnp.bfloat16
H = 3


def act(gate, up):
    return jax.nn.gelu(gate) * up


def dot(a, b, ca, cb):
    return lax.dot_general(a, b, (((ca,), (cb,)), ((), ())), preferred_element_type=F32)


def tile_of(n, cap):
    return max(t for t in range(128, min(n, cap) + 1, 128) if n % t == 0)


MID_M = {0: 0, 1: 1, -1: 2, 2: 3}


def kernel(x_ref, dy_ref, gate_ref, up_ref, wg_ref, wu_ref, wd_ref,
           base_ref, dwg_ref, dwu_ref, dwd_ref, rw, wlast,
           dyg, xg, dgs, dus, pown, pin, tst, ru, rv, rso,
           xv, gv, uv, pc, tc, rc, sc, oc, fc,
           sF, sE, rF, rE, sP, rP, sT, rT, sU, rU, sV, rV, sW, rW, lsem):
    S, D = x_ref.shape
    F = gate_ref.shape[1]
    C = S // H
    tp = lax.axis_index("tp")
    z, c = tp // 2, tp % 2
    way = jnp.where(z < 2, 1, -1)
    is_end = (z == 0) | (z == 3)
    is_mid = (z == 1) | (z == 2)

    def chip(k):
        return z + way * k

    def dev(k):
        return {"tp": 2 * chip(k) + c}

    partner = {"tp": 2 * z + 1 - c}
    rows = lambda h: pl.ds(h * C, C)
    given, gathered = (dy_ref, x_ref), (dyg, xg)

    def rcopy(src, dst, ssem, rsem, to):
        return pltpu.make_async_remote_copy(
            src_ref=src, dst_ref=dst, send_sem=ssem, recv_sem=rsem, device_id=to, device_id_type=MESH)

    def local(*copies):
        made = [pltpu.make_async_copy(s, d, lsem.at[i]) for i, (s, d) in enumerate(copies)]
        for cp in made:
            cp.start()
        for cp in made:
            cp.wait()

    def piece(a, k, h):
        return gathered[a].at[2 * chip(k) + c, rows(h)]

    def source(a, k, h):
        return given[a].at[rows(h)] if k == 0 else piece(a, k, h)

    def end_to_f(a, h):
        return rcopy(source(a, 0, h), piece(a, 0, h), sF.at[a, 0, h], rE.at[a, h], dev(1))

    def mid_to_f(a, k, h):
        j = 0 if k == 0 else 1
        return rcopy(source(a, k, h), piece(a, k, h), sF.at[a, j, h], rF.at[a, j, h], dev(1))

    def mid_to_e(a, k, h):
        return rcopy(source(a, k, h), piece(a, k, h), sE.at[a, k, h], rF.at[a, k, h], dev(-1))

    def to_partner(a, k, m):
        src = given[a] if k == 0 else gathered[a].at[2 * chip(k) + c]
        return rcopy(src, gathered[a].at[2 * chip(k) + c], sP.at[a, m], rP.at[a, m], partner)

    def wait_f(a, k, h):
        rcopy(piece(a, k, h), piece(a, k, h), sF.at[a, 0, h], rF.at[a, k - 1, h], partner).wait_recv()

    def wait_e(a, h):
        rcopy(piece(a, -1, h), piece(a, -1, h), sF.at[a, 0, h], rE.at[a, h], partner).wait_recv()

    def term(m):
        return rcopy(tst.at[m], pin.at[m], sT.at[m], rT.at[m], partner)

    def u_copy(j, h):
        return rcopy(rso.at[j, rows(h)], ru.at[j, rows(h)], sU.at[j, h], rU.at[j, h], dev(1))

    def v_copy(j, h):
        return rcopy(rso.at[j, rows(h)], rv.at[j, rows(h)], sV.at[j, h], rV.at[j, h], dev(1))

    def w_copy(h):
        return rcopy(rso.at[2, rows(h)], rw.at[rows(h)], sW.at[h], rW.at[h], dev(-1))

    def combine(m, h, received, out, res=oc):
        bufs = [pc, tc, rc, sc]
        srcs = [pown.at[m, rows(h)], pin.at[m, rows(h)], *received]
        local(*zip(srcs, bufs))
        step = 16

        @pl.loop(0, C // step)
        def _(i):
            r = pl.ds(pl.multiple_of(i * step, step), step)
            total = pc[r, :] + tc[r, :].astype(F32)
            for b in bufs[2:len(srcs)]:
                total += b[r, :].astype(F32)
            res[r, :] = total.astype(res.dtype)

        local((res, out))

    barrier = pltpu.get_barrier_semaphore()
    pl.semaphore_signal(barrier, inc=1, device_id=partner, device_id_type=MESH)
    pl.semaphore_signal(barrier, inc=1, device_id=dev(1), device_id_type=MESH)

    @pl.when(is_mid)
    def _():
        pl.semaphore_signal(barrier, inc=1, device_id=dev(-1), device_id_type=MESH)
        pl.semaphore_wait(barrier, 3)

    @pl.when(is_end)
    def _():
        pl.semaphore_wait(barrier, 2)

    @pl.when(is_mid)
    def _():
        for h in range(H):
            mid_to_e(0, 0, h).start()
            mid_to_f(0, 0, h).start()

    @pl.when(is_end)
    def _():
        for h in range(H):
            end_to_f(0, h).start()
        for h in range(H):
            end_to_f(1, h).start()

    for a in range(2):
        to_partner(a, 0, 0).start()

    def k_of(m):
        mid = jnp.where(m == 2, -1, jnp.where(m == 3, 2, m))
        return jnp.where(is_end, m, mid)

    def load_shard(a, m, p):
        t = 2 * (z + way * k_of(m)) + jnp.where(p == 0, c, 1 - c)

        @pl.when(p == 1)
        def _():
            rcopy(gathered[a].at[t], gathered[a].at[t], sP.at[a, m], rP.at[a, m], partner).wait_recv()

        @pl.when((m == 0) & (p == 0))
        def _():
            pltpu.make_async_copy(given[a], xv, lsem.at[2]).start()

        @pl.when((m > 0) | (p > 0))
        def _():
            pltpu.make_async_copy(gathered[a].at[t], xv, lsem.at[2]).start()

        return t

    def phase1(wd, wg, wu, accd, hid, dgv, duv, dxf, dxb, stage):
        local((wd_ref, wd), (wg_ref, wg))
        local((wu_ref, wu))
        accd[...] = jnp.zeros_like(accd)

        def unit(m, p):
            t = load_shard(0, m, p)
            local((gate_ref.at[pl.ds(t * S, S)], gv), (up_ref.at[pl.ds(t * S, S)], uv))
            pltpu.make_async_copy(given[0], xv, lsem.at[2]).wait()
            tn = min(F, 256)

            @pl.loop(0, pl.cdiv(F, tn))
            def _(n):
                s = pl.ds(pl.multiple_of(jnp.minimum(n * tn, F - tn), 128), tn)
                d_hidden = dot(xv[...], wd[s, :], 1, 1)
                hidden, back = jax.vjp(act, gv[:, s].astype(F32), uv[:, s].astype(F32))
                d_gate, d_up = back(d_hidden)
                hid[:, s] = hidden.astype(BF16)
                dgv[:, s] = d_gate.astype(BF16)
                duv[:, s] = d_up.astype(BF16)

            keep = [pltpu.make_async_copy(v, o.at[2 * m + p], lsem.at[i])
                    for i, (v, o) in enumerate(((dgv, dgs), (duv, dus)))]
            for cp in keep:
                cp.start()
            tn2 = tile_of(D, 256)

            @pl.loop(0, D // tn2)
            def _(n):
                s = pl.ds(pl.multiple_of(n * tn2, tn2), tn2)
                part = dot(dgv[...], wg[s, :], 1, 1) + dot(duv[...], wu[s, :], 1, 1)
                dxf[:, s] = part
                dxb[:, s] = part.astype(BF16)

            for cp in keep:
                cp.wait()

            @pl.when(p == 0)
            def _():
                local((dxf, pown.at[m]))

            @pl.when(p == 1)
            def _():
                local((dxb, tst.at[m]))
                term(m).start()

            tn3 = tile_of(D, 768)

            @pl.loop(0, D // tn3)
            def _(n):
                s = pl.ds(pl.multiple_of(n * tn3, tn3), tn3)
                accd[:, s] += dot(hid[...], xv[:, s], 0, 0)

        def wait_term(m):
            term(m).wait_recv()

        def send_u(j):
            wait_term(j + 1)
            for h in range(H):
                combine(j + 1, h, [], rso.at[j, rows(h)])
                u_copy(j, h).start()

        @pl.loop(0, 4)
        def _(m):
            @pl.loop(0, 2)
            def _(p):
                unit(m, p)

            @pl.when((m == 0) & is_end)
            def _():
                for h in range(H):
                    wait_f(0, 1, h)
                to_partner(0, 1, 1).start()

            @pl.when((m == 0) & is_mid)
            def _():
                for h in range(H):
                    wait_f(0, 1, h)
                    mid_to_e(0, 1, h).start()
                    wait_e(0, h)
                    mid_to_f(0, -1, h).start()
                to_partner(0, 1, 1).start()
                to_partner(0, -1, 2).start()
                for h in range(H):
                    mid_to_f(1, 0, h).start()

            @pl.when((m == 1) & is_end)
            def _():
                send_u(0)
                for h in range(H):
                    wait_f(0, 2, h)
                to_partner(0, 2, 2).start()

            @pl.when((m == 1) & is_mid)
            def _():
                for h in range(H):
                    wait_f(0, 2, h)
                    mid_to_e(0, 2, h).start()
                to_partner(0, 2, 3).start()
                for h in range(H):
                    mid_to_e(1, 0, h).start()
                for h in range(H):
                    wait_e(1, h)
                    mid_to_f(1, -1, h).start()
                to_partner(1, -1, 2).start()

            @pl.when((m == 2) & is_end)
            def _():
                send_u(1)
                for h in range(H):
                    wait_f(0, 3, h)
                to_partner(0, 3, 3).start()

            @pl.when((m == 2) & is_mid)
            def _():
                for h in range(H):
                    wait_f(1, 1, h)
                    mid_to_e(1, 1, h).start()
                to_partner(1, 1, 1).start()

            @pl.when((m == 3) & is_end)
            def _():
                send_u(2)

        flush([(accd, dwd_ref)], stage)

    def flush(pairs, stage):
        n = stage.shape[1]
        jobs = [(acc, out, r) for acc, out in pairs for r in range(0, acc.shape[0], n)]
        made = []
        for i, (acc, out, r) in enumerate(jobs):
            if i >= 2:
                made[i - 2].wait()
            stage[i % 2] = acc[r:r + n, :].astype(BF16)
            made.append(pltpu.make_async_copy(stage.at[i % 2], out.at[pl.ds(r, n)], lsem.at[i % 2]))
            made[i].start()
        for cp in made[-2:]:
            cp.wait()

    def own_rows():
        term(0).wait_recv()

        @pl.when(is_mid)
        def _():
            for h in range(H):
                rcopy(ru.at[0, rows(h)], ru.at[0, rows(h)], sU.at[0, h], rU.at[0, h], partner).wait_recv()
                rcopy(rv.at[0, rows(h)], rv.at[0, rows(h)], sV.at[0, h], rV.at[0, h], partner).wait_recv()
                combine(0, h, [ru.at[0, rows(h)], rv.at[0, rows(h)]], base_ref.at[rows(h)], fc)

        @pl.when(is_end)
        def _():
            for h in range(H):
                combine(0, h, [], base_ref.at[rows(h)], fc)

    def send_v(j):
        m = MID_M[j + 1]
        term(m).wait_recv()
        for h in range(H):
            rcopy(ru.at[j + 1, rows(h)], ru.at[j + 1, rows(h)], sU.at[j + 1, h], rU.at[j + 1, h], partner).wait_recv()
            combine(m, h, [ru.at[j + 1, rows(h)]], rso.at[j, rows(h)])
            v_copy(j, h).start()

    def send_w():
        m = MID_M[-1]
        term(m).wait_recv()
        for h in range(H):
            rcopy(rv.at[1, rows(h)], rv.at[1, rows(h)], sV.at[1, h], rV.at[1, h], partner).wait_recv()
            combine(m, h, [rv.at[1, rows(h)]], rso.at[2, rows(h)] if h < H - 1 else wlast)
            if h < H - 1:
                w_copy(h).start()

    def phase2(accg, accu, stage):
        accg[...] = jnp.zeros_like(accg)
        accu[...] = jnp.zeros_like(accu)

        def unit(m, p):
            load_shard(1, m, p)
            local((dgs.at[2 * m + p], gv), (dus.at[2 * m + p], uv))
            pltpu.make_async_copy(given[1], xv, lsem.at[2]).wait()
            tm = tile_of(D, 768)

            @pl.loop(0, D // tm)
            def _(n):
                s = pl.ds(pl.multiple_of(n * tm, tm), tm)
                accg[s, :] += dot(xv[:, s], gv[...], 0, 0)
                accu[s, :] += dot(xv[:, s], uv[...], 0, 0)

        @pl.loop(0, 4)
        def _(m):
            @pl.when((m == 0) & is_mid)
            def _():
                send_v(0)

            @pl.when((m == 1) & is_mid)
            def _():
                for h in range(H):
                    wait_f(1, 2, h)
                    mid_to_e(1, 2, h).start()
                to_partner(1, 2, 3).start()

            @pl.when((m == 3) & is_mid)
            def _():
                send_v(1)

            @pl.when(m == 3)
            def _():
                own_rows()

            for i in range(1, 4):
                @pl.when((m == i) & is_end)
                def _(i=i):
                    for h in range(H):
                        wait_f(1, i, h)
                    to_partner(1, i, i).start()

            @pl.loop(0, 2)
            def _(p):
                unit(m, p)

        @pl.when(is_mid)
        def _():
            send_w()

        flush([(accg, dwg_ref), (accu, dwu_ref)], stage)

    wbuf = lambda r: pltpu.VMEM(r.shape, r.dtype)
    pl.run_scoped(
        phase1, wbuf(wd_ref), wbuf(wg_ref), wbuf(wu_ref), pltpu.VMEM((F, D), F32),
        pltpu.VMEM((S, F), BF16), pltpu.VMEM((S, F), BF16), pltpu.VMEM((S, F), BF16),
        pltpu.VMEM((S, D), F32), pltpu.VMEM((S, D), BF16), pltpu.VMEM((2, tile_of(F, 128), D), BF16))
    pl.run_scoped(
        phase2, pltpu.VMEM((D, F), F32), pltpu.VMEM((D, F), F32), pltpu.VMEM((2, tile_of(D, 256), F), BF16))

    @pl.when(is_end)
    def _():
        for h in range(H - 1):
            rcopy(rw.at[rows(h)], rw.at[rows(h)], sW.at[h], rW.at[h], partner).wait_recv()

    for m in range(4):
        term(m).wait_send()

    @pl.when(is_end)
    def _():
        for a in range(2):
            for h in range(H):
                end_to_f(a, h).wait_send()
            for k in range(4):
                to_partner(a, k, k).wait_send()
        for j in range(3):
            for h in range(H):
                u_copy(j, h).wait_send()

    @pl.when(is_mid)
    def _():
        for a in range(2):
            for h in range(H):
                for k in (0, 1, 2):
                    mid_to_e(a, k, h).wait_send()
                for k in (0, -1):
                    mid_to_f(a, k, h).wait_send()
            for k, m in MID_M.items():
                to_partner(a, k, m).wait_send()
        for h in range(H):
            for j in range(2):
                v_copy(j, h).wait_send()
        for h in range(H - 1):
            w_copy(h).wait_send()


def finish_kernel(base, part, gate_in, up_in, down_in, dx, gate_out, up_out, down_out, gv, uv, dv, bv, pv, ov, isem, osem):
    n = part.shape[0]
    bring = [pltpu.make_async_copy(base.at[pl.ds(0, n)], bv, isem.at[0]), pltpu.make_async_copy(part, pv, isem.at[1])]
    put = []
    for src, v, dst in ((gate_in, gv, gate_out), (up_in, uv, up_out), (down_in, dv, down_out)):
        size = src.shape[0] // 3
        for r in range(3):
            piece = pl.ds(r * size, size)
            bring.append(pltpu.make_async_copy(src.at[piece], v.at[piece], isem.at[len(bring)]))
            put.append(pltpu.make_async_copy(v.at[piece], dst.at[piece], osem.at[len(put)]))
    for cp in bring:
        cp.start()
    bring[0].wait()
    bring[1].wait()
    tp = lax.axis_index("tp")
    is_end = (tp < 2) | (tp >= 6)
    step = 16

    @pl.loop(0, n // step)
    def _(i):
        r = pl.ds(pl.multiple_of(i * step, step), step)
        ov[r, :] = (bv[r, :] + jnp.where(is_end, pv[r, :].astype(F32), 0.0)).astype(BF16)

    put.append(pltpu.make_async_copy(ov, dx.at[pl.ds(0, n)], osem.at[len(put)]))
    put[-1].start()
    for got, cp in zip(bring[2:], put):
        got.wait()
        cp.start()
    for cp in put:
        cp.wait()


def finish(base, part, *grads):
    S, D = base.shape
    any_ = pl.BlockSpec(memory_space=pl.ANY)
    n = part.shape[0]
    moved = 2 * sum(g.size * 2 for g in grads)
    return pl.pallas_call(
        finish_kernel, in_specs=[any_] * 5, out_specs=[any_] * 4,
        out_shape=[jax.ShapeDtypeStruct((S, D), BF16)] + [jax.ShapeDtypeStruct(g.shape, BF16) for g in grads],
        scratch_shapes=[pltpu.VMEM(g.shape, BF16) for g in grads] + [
            pltpu.VMEM((n, D), F32), pltpu.VMEM((n, D), BF16), pltpu.VMEM((n, D), BF16),
            pltpu.SemaphoreType.DMA((11,)), pltpu.SemaphoreType.DMA((10,))],
        compiler_params=pltpu.CompilerParams(vmem_limit_bytes=62 * 2**20),
        cost_estimate=pl.CostEstimate(flops=10**9, bytes_accessed=moved, transcendentals=0),
        name="finish")(base, part, *grads)


def solution(mesh):
    def step(x, dy, gate, up, w_gate, w_up, w_down):
        (S, D), F = x.shape, gate.shape[1]
        C = S // H
        shape = jax.ShapeDtypeStruct
        any_ = pl.BlockSpec(memory_space=pl.ANY)
        outs = [
            shape((S, D), F32), shape((D, F), BF16), shape((D, F), BF16), shape((F, D), BF16),
            shape((S - C, D), BF16), shape((C, D), BF16),
            shape((8, S, D), BF16), shape((8, S, D), BF16),
            shape((8, S, F), BF16), shape((8, S, F), BF16),
            shape((4, S, D), F32), shape((4, S, D), BF16), shape((4, S, D), BF16),
            shape((3, S, D), BF16), shape((2, S, D), BF16), shape((3, S, D), BF16),
        ]
        dma = pltpu.SemaphoreType.DMA
        out = pl.pallas_call(
            kernel,
            out_shape=outs,
            in_specs=[any_] * 7,
            out_specs=[any_] * len(outs),
            scratch_shapes=[
                pltpu.VMEM((S, D), BF16), pltpu.VMEM((S, F), BF16), pltpu.VMEM((S, F), BF16),
                pltpu.VMEM((C, D), F32), pltpu.VMEM((C, D), BF16), pltpu.VMEM((C, D), BF16),
                pltpu.VMEM((C, D), BF16), pltpu.VMEM((C, D), BF16), pltpu.VMEM((C, D), F32),
                dma((2, 2, H)), dma((2, 3, H)), dma((2, 3, H)), dma((2, H)),
                dma((2, 4)), dma((2, 4)), dma((4,)), dma((4,)),
                dma((3, H)), dma((3, H)), dma((2, H)), dma((2, H)), dma((H,)), dma((H,)),
                dma((4,)),
            ],
            compiler_params=pltpu.CompilerParams(
                collective_id=0, has_side_effects=True, vmem_limit_bytes=60 * 2**20),
            name="mlp_backward",
        )(x, dy, gate, up, w_gate, w_up, w_down)
        base, dwg, dwu, dwd, early, last = out[:6]
        last = lax.ppermute(last, "tp", [(2, 0), (3, 1), (4, 6), (5, 7)])
        dx, *grads = finish(base, early, dwg, dwu, dwd)
        done = S - C
        dx = lax.dynamic_update_slice(dx, (base[done:] + last.astype(F32)).astype(BF16), (done, 0))
        return dx, *grads

    both = P(("dp", "tp"), None)
    cols = P("dp", "tp")
    return jax.shard_map(
        step, mesh=mesh,
        in_specs=(both, both, cols, cols, P(None, "tp"), P(None, "tp"), P("tp", None)),
        out_specs=(both, cols, cols, both), check_vma=False)
```

```python
import functools

import jax
import jax.numpy as jnp
from jax import lax
from jax.experimental import pallas as pl
from jax.experimental.pallas import tpu as pltpu
from jax.sharding import PartitionSpec as P

MESH = pl.DeviceIdType.MESH
F32, BF16 = jnp.float32, jnp.bfloat16
H = 3


def act(gate, up):
    return jax.nn.gelu(gate) * up


def dot(a, b, ca, cb):
    return lax.dot_general(a, b, (((ca,), (cb,)), ((), ())), preferred_element_type=F32)


def tile_of(n, cap):
    return max(t for t in range(128, min(n, cap) + 1, 128) if n % t == 0)


MID_M = {0: 0, 1: 1, -1: 2, 2: 3}


def kernel(x_ref, dy_ref, gate_ref, up_ref, wg_ref, wu_ref, wd_ref,
           base_ref, dwg_ref, dwu_ref, dwd_ref, rw, wlast,
           dyg, xg, dgs, dus, pown, pin, tst, ru, rv, rso,
           xv, gv, uv, pc, tc, rc, sc, oc, fc,
           sF, sE, rF, rE, sP, rP, sT, rT, sU, rU, sV, rV, sW, rW, lsem):
    S, D = x_ref.shape
    F = gate_ref.shape[1]
    C = S // H
    tp = lax.axis_index("tp")
    z, c = tp // 2, tp % 2
    way = jnp.where(z < 2, 1, -1)
    is_end = (z == 0) | (z == 3)
    is_mid = (z == 1) | (z == 2)

    def chip(k):
        return z + way * k

    def dev(k):
        return {"tp": 2 * chip(k) + c}

    partner = {"tp": 2 * z + 1 - c}
    rows = lambda h: pl.ds(h * C, C)
    given, gathered = (dy_ref, x_ref), (dyg, xg)

    def rcopy(src, dst, ssem, rsem, to):
        return pltpu.make_async_remote_copy(
            src_ref=src, dst_ref=dst, send_sem=ssem, recv_sem=rsem, device_id=to, device_id_type=MESH)

    def local(*copies):
        made = [pltpu.make_async_copy(s, d, lsem.at[i]) for i, (s, d) in enumerate(copies)]
        for cp in made:
            cp.start()
        for cp in made:
            cp.wait()

    def piece(a, k, h):
        return gathered[a].at[2 * chip(k) + c, rows(h)]

    def source(a, k, h):
        return given[a].at[rows(h)] if k == 0 else piece(a, k, h)

    def end_to_f(a, h):
        return rcopy(source(a, 0, h), piece(a, 0, h), sF.at[a, 0, h], rE.at[a, h], dev(1))

    def mid_to_f(a, k, h):
        j = 0 if k == 0 else 1
        return rcopy(source(a, k, h), piece(a, k, h), sF.at[a, j, h], rF.at[a, j, h], dev(1))

    def mid_to_e(a, k, h):
        return rcopy(source(a, k, h), piece(a, k, h), sE.at[a, k, h], rF.at[a, k, h], dev(-1))

    def to_partner(a, k, m):
        src = given[a] if k == 0 else gathered[a].at[2 * chip(k) + c]
        return rcopy(src, gathered[a].at[2 * chip(k) + c], sP.at[a, m], rP.at[a, m], partner)

    def wait_f(a, k, h):
        rcopy(piece(a, k, h), piece(a, k, h), sF.at[a, 0, h], rF.at[a, k - 1, h], partner).wait_recv()

    def wait_e(a, h):
        rcopy(piece(a, -1, h), piece(a, -1, h), sF.at[a, 0, h], rE.at[a, h], partner).wait_recv()

    def term(m):
        return rcopy(tst.at[m], pin.at[m], sT.at[m], rT.at[m], partner)

    def u_copy(j, h):
        return rcopy(rso.at[j, rows(h)], ru.at[j, rows(h)], sU.at[j, h], rU.at[j, h], dev(1))

    def v_copy(j, h):
        return rcopy(rso.at[j, rows(h)], rv.at[j, rows(h)], sV.at[j, h], rV.at[j, h], dev(1))

    def w_copy(h):
        return rcopy(rso.at[2, rows(h)], rw.at[rows(h)], sW.at[h], rW.at[h], dev(-1))

    def combine(m, h, received, out, res=oc):
        bufs = [pc, tc, rc, sc]
        srcs = [pown.at[m, rows(h)], pin.at[m, rows(h)], *received]
        local(*zip(srcs, bufs))
        step = 16

        @pl.loop(0, C // step)
        def _(i):
            r = pl.ds(pl.multiple_of(i * step, step), step)
            total = pc[r, :] + tc[r, :].astype(F32)
            for b in bufs[2:len(srcs)]:
                total += b[r, :].astype(F32)
            res[r, :] = total.astype(res.dtype)

        local((res, out))

    barrier = pltpu.get_barrier_semaphore()
    pl.semaphore_signal(barrier, inc=1, device_id=partner, device_id_type=MESH)
    pl.semaphore_signal(barrier, inc=1, device_id=dev(1), device_id_type=MESH)

    @pl.when(is_mid)
    def _():
        pl.semaphore_signal(barrier, inc=1, device_id=dev(-1), device_id_type=MESH)
        pl.semaphore_wait(barrier, 3)

    @pl.when(is_end)
    def _():
        pl.semaphore_wait(barrier, 2)

    @pl.when(is_mid)
    def _():
        for h in range(H):
            mid_to_e(0, 0, h).start()
            mid_to_f(0, 0, h).start()

    @pl.when(is_end)
    def _():
        for h in range(H):
            end_to_f(0, h).start()
        for h in range(H):
            end_to_f(1, h).start()

    for a in range(2):
        to_partner(a, 0, 0).start()

    def k_of(m):
        mid = jnp.where(m == 2, -1, jnp.where(m == 3, 2, m))
        return jnp.where(is_end, m, mid)

    def load_shard(a, m, p):
        t = 2 * (z + way * k_of(m)) + jnp.where(p == 0, c, 1 - c)

        @pl.when(p == 1)
        def _():
            rcopy(gathered[a].at[t], gathered[a].at[t], sP.at[a, m], rP.at[a, m], partner).wait_recv()

        @pl.when((m == 0) & (p == 0))
        def _():
            pltpu.make_async_copy(given[a], xv, lsem.at[2]).start()

        @pl.when((m > 0) | (p > 0))
        def _():
            pltpu.make_async_copy(gathered[a].at[t], xv, lsem.at[2]).start()

        return t

    def phase1(wd, wg, wu, accd, hid, dgv, duv, dxf, dxb, stage):
        local((wd_ref, wd), (wg_ref, wg))
        local((wu_ref, wu))
        accd[...] = jnp.zeros_like(accd)

        def unit(m, p):
            t = load_shard(0, m, p)
            local((gate_ref.at[pl.ds(t * S, S)], gv), (up_ref.at[pl.ds(t * S, S)], uv))
            pltpu.make_async_copy(given[0], xv, lsem.at[2]).wait()
            tn = min(F, 256)

            @pl.loop(0, pl.cdiv(F, tn))
            def _(n):
                s = pl.ds(pl.multiple_of(jnp.minimum(n * tn, F - tn), 128), tn)
                d_hidden = dot(xv[...], wd[s, :], 1, 1)
                hidden, back = jax.vjp(act, gv[:, s].astype(F32), uv[:, s].astype(F32))
                d_gate, d_up = back(d_hidden)
                hid[:, s] = hidden.astype(BF16)
                dgv[:, s] = d_gate.astype(BF16)
                duv[:, s] = d_up.astype(BF16)

            keep = [pltpu.make_async_copy(v, o.at[2 * m + p], lsem.at[i])
                    for i, (v, o) in enumerate(((dgv, dgs), (duv, dus)))]
            for cp in keep:
                cp.start()
            tn2 = tile_of(D, 256)

            @pl.loop(0, D // tn2)
            def _(n):
                s = pl.ds(pl.multiple_of(n * tn2, tn2), tn2)
                part = dot(dgv[...], wg[s, :], 1, 1) + dot(duv[...], wu[s, :], 1, 1)
                dxf[:, s] = part
                dxb[:, s] = part.astype(BF16)

            for cp in keep:
                cp.wait()

            @pl.when(p == 0)
            def _():
                local((dxf, pown.at[m]))

            @pl.when(p == 1)
            def _():
                local((dxb, tst.at[m]))
                term(m).start()

            tn3 = tile_of(D, 768)

            @pl.loop(0, D // tn3)
            def _(n):
                s = pl.ds(pl.multiple_of(n * tn3, tn3), tn3)
                accd[:, s] += dot(hid[...], xv[:, s], 0, 0)

        def wait_term(m):
            term(m).wait_recv()

        def send_u(j):
            wait_term(j + 1)
            for h in range(H):
                combine(j + 1, h, [], rso.at[j, rows(h)])
                u_copy(j, h).start()

        @pl.loop(0, 4)
        def _(m):
            @pl.loop(0, 2)
            def _(p):
                unit(m, p)

            @pl.when((m == 0) & is_end)
            def _():
                for h in range(H):
                    wait_f(0, 1, h)
                to_partner(0, 1, 1).start()

            @pl.when((m == 0) & is_mid)
            def _():
                for h in range(H):
                    wait_f(0, 1, h)
                    mid_to_e(0, 1, h).start()
                    wait_e(0, h)
                    mid_to_f(0, -1, h).start()
                to_partner(0, 1, 1).start()
                to_partner(0, -1, 2).start()
                for h in range(H):
                    mid_to_f(1, 0, h).start()

            @pl.when((m == 1) & is_end)
            def _():
                send_u(0)
                for h in range(H):
                    wait_f(0, 2, h)
                to_partner(0, 2, 2).start()

            @pl.when((m == 1) & is_mid)
            def _():
                for h in range(H):
                    wait_f(0, 2, h)
                    mid_to_e(0, 2, h).start()
                to_partner(0, 2, 3).start()
                for h in range(H):
                    mid_to_e(1, 0, h).start()
                for h in range(H):
                    wait_e(1, h)
                    mid_to_f(1, -1, h).start()
                to_partner(1, -1, 2).start()

            @pl.when((m == 2) & is_end)
            def _():
                send_u(1)
                for h in range(H):
                    wait_f(0, 3, h)
                to_partner(0, 3, 3).start()

            @pl.when((m == 2) & is_mid)
            def _():
                for h in range(H):
                    wait_f(1, 1, h)
                    mid_to_e(1, 1, h).start()
                to_partner(1, 1, 1).start()

            @pl.when((m == 3) & is_end)
            def _():
                send_u(2)

        flush([(accd, dwd_ref)], stage)

    def flush(pairs, stage):
        n = stage.shape[1]
        jobs = [(acc, out, r) for acc, out in pairs for r in range(0, acc.shape[0], n)]
        made = []
        for i, (acc, out, r) in enumerate(jobs):
            if i >= 2:
                made[i - 2].wait()
            stage[i % 2] = acc[r:r + n, :].astype(BF16)
            made.append(pltpu.make_async_copy(stage.at[i % 2], out.at[pl.ds(r, n)], lsem.at[i % 2]))
            made[i].start()
        for cp in made[-2:]:
            cp.wait()

    def own_rows():
        term(0).wait_recv()

        @pl.when(is_mid)
        def _():
            for h in range(H):
                rcopy(ru.at[0, rows(h)], ru.at[0, rows(h)], sU.at[0, h], rU.at[0, h], partner).wait_recv()
                rcopy(rv.at[0, rows(h)], rv.at[0, rows(h)], sV.at[0, h], rV.at[0, h], partner).wait_recv()
                combine(0, h, [ru.at[0, rows(h)], rv.at[0, rows(h)]], base_ref.at[rows(h)], fc)

        @pl.when(is_end)
        def _():
            for h in range(H):
                combine(0, h, [], base_ref.at[rows(h)], fc)

    def send_v(j):
        m = MID_M[j + 1]
        term(m).wait_recv()
        for h in range(H):
            rcopy(ru.at[j + 1, rows(h)], ru.at[j + 1, rows(h)], sU.at[j + 1, h], rU.at[j + 1, h], partner).wait_recv()
            combine(m, h, [ru.at[j + 1, rows(h)]], rso.at[j, rows(h)])
            v_copy(j, h).start()

    def send_w():
        m = MID_M[-1]
        term(m).wait_recv()
        for h in range(H):
            rcopy(rv.at[1, rows(h)], rv.at[1, rows(h)], sV.at[1, h], rV.at[1, h], partner).wait_recv()
            combine(m, h, [rv.at[1, rows(h)]], rso.at[2, rows(h)] if h < H - 1 else wlast)
            if h < H - 1:
                w_copy(h).start()

    def phase2(accg, accu, stage):
        accg[...] = jnp.zeros_like(accg)
        accu[...] = jnp.zeros_like(accu)

        def unit(m, p):
            load_shard(1, m, p)
            local((dgs.at[2 * m + p], gv), (dus.at[2 * m + p], uv))
            pltpu.make_async_copy(given[1], xv, lsem.at[2]).wait()
            tm = tile_of(D, 768)

            @pl.loop(0, D // tm)
            def _(n):
                s = pl.ds(pl.multiple_of(n * tm, tm), tm)
                accg[s, :] += dot(xv[:, s], gv[...], 0, 0)
                accu[s, :] += dot(xv[:, s], uv[...], 0, 0)

        @pl.loop(0, 4)
        def _(m):
            @pl.when((m == 0) & is_mid)
            def _():
                send_v(0)

            @pl.when((m == 1) & is_mid)
            def _():
                for h in range(H):
                    wait_f(1, 2, h)
                    mid_to_e(1, 2, h).start()
                to_partner(1, 2, 3).start()

            @pl.when((m == 2) & is_mid)
            def _():
                send_v(1)

            @pl.when((m == 3) & is_end)
            def _():
                own_rows()

            for i in range(1, 4):
                @pl.when((m == i) & is_end)
                def _(i=i):
                    for h in range(H):
                        wait_f(1, i, h)
                    to_partner(1, i, i).start()

            @pl.loop(0, 2)
            def _(p):
                unit(m, p)

        @pl.when(is_mid)
        def _():
            send_w()
            own_rows()

        flush([(accg, dwg_ref), (accu, dwu_ref)], stage)

    wbuf = lambda r: pltpu.VMEM(r.shape, r.dtype)
    pl.run_scoped(
        phase1, wbuf(wd_ref), wbuf(wg_ref), wbuf(wu_ref), pltpu.VMEM((F, D), F32),
        pltpu.VMEM((S, F), BF16), pltpu.VMEM((S, F), BF16), pltpu.VMEM((S, F), BF16),
        pltpu.VMEM((S, D), F32), pltpu.VMEM((S, D), BF16), pltpu.VMEM((2, tile_of(F, 128), D), BF16))
    pl.run_scoped(
        phase2, pltpu.VMEM((D, F), F32), pltpu.VMEM((D, F), F32), pltpu.VMEM((2, tile_of(D, 256), F), BF16))

    @pl.when(is_end)
    def _():
        for h in range(H - 1):
            rcopy(rw.at[rows(h)], rw.at[rows(h)], sW.at[h], rW.at[h], partner).wait_recv()

    for m in range(4):
        term(m).wait_send()

    @pl.when(is_end)
    def _():
        for a in range(2):
            for h in range(H):
                end_to_f(a, h).wait_send()
            for k in range(4):
                to_partner(a, k, k).wait_send()
        for j in range(3):
            for h in range(H):
                u_copy(j, h).wait_send()

    @pl.when(is_mid)
    def _():
        for a in range(2):
            for h in range(H):
                for k in (0, 1, 2):
                    mid_to_e(a, k, h).wait_send()
                for k in (0, -1):
                    mid_to_f(a, k, h).wait_send()
            for k, m in MID_M.items():
                to_partner(a, k, m).wait_send()
        for h in range(H):
            for j in range(2):
                v_copy(j, h).wait_send()
        for h in range(H - 1):
            w_copy(h).wait_send()


def finish_kernel(base, part, gate_in, up_in, down_in, dx, gate_out, up_out, down_out, gv, uv, dv, bv, pv, ov, isem, osem):
    n = part.shape[0]
    bring = [pltpu.make_async_copy(base.at[pl.ds(0, n)], bv, isem.at[0]), pltpu.make_async_copy(part, pv, isem.at[1])]
    put = []
    for src, v, dst in ((gate_in, gv, gate_out), (up_in, uv, up_out), (down_in, dv, down_out)):
        size = src.shape[0] // 3
        for r in range(3):
            piece = pl.ds(r * size, size)
            bring.append(pltpu.make_async_copy(src.at[piece], v.at[piece], isem.at[len(bring)]))
            put.append(pltpu.make_async_copy(v.at[piece], dst.at[piece], osem.at[len(put)]))
    for cp in bring:
        cp.start()
    bring[0].wait()
    bring[1].wait()
    tp = lax.axis_index("tp")
    is_end = (tp < 2) | (tp >= 6)
    step = 16

    @pl.loop(0, n // step)
    def _(i):
        r = pl.ds(pl.multiple_of(i * step, step), step)
        ov[r, :] = (bv[r, :] + jnp.where(is_end, pv[r, :].astype(F32), 0.0)).astype(BF16)

    put.append(pltpu.make_async_copy(ov, dx.at[pl.ds(0, n)], osem.at[len(put)]))
    put[-1].start()
    for got, cp in zip(bring[2:], put):
        got.wait()
        cp.start()
    for cp in put:
        cp.wait()


def finish(base, part, *grads):
    S, D = base.shape
    any_ = pl.BlockSpec(memory_space=pl.ANY)
    n = part.shape[0]
    moved = 2 * sum(g.size * 2 for g in grads)
    return pl.pallas_call(
        finish_kernel, in_specs=[any_] * 5, out_specs=[any_] * 4,
        out_shape=[jax.ShapeDtypeStruct((S, D), BF16)] + [jax.ShapeDtypeStruct(g.shape, BF16) for g in grads],
        scratch_shapes=[pltpu.VMEM(g.shape, BF16) for g in grads] + [
            pltpu.VMEM((n, D), F32), pltpu.VMEM((n, D), BF16), pltpu.VMEM((n, D), BF16),
            pltpu.SemaphoreType.DMA((11,)), pltpu.SemaphoreType.DMA((10,))],
        compiler_params=pltpu.CompilerParams(vmem_limit_bytes=62 * 2**20),
        cost_estimate=pl.CostEstimate(flops=10**9, bytes_accessed=moved, transcendentals=0),
        name="finish")(base, part, *grads)


def solution(mesh):
    def step(x, dy, gate, up, w_gate, w_up, w_down):
        (S, D), F = x.shape, gate.shape[1]
        C = S // H
        shape = jax.ShapeDtypeStruct
        any_ = pl.BlockSpec(memory_space=pl.ANY)
        outs = [
            shape((S, D), F32), shape((D, F), BF16), shape((D, F), BF16), shape((F, D), BF16),
            shape((S - C, D), BF16), shape((C, D), BF16),
            shape((8, S, D), BF16), shape((8, S, D), BF16),
            shape((8, S, F), BF16), shape((8, S, F), BF16),
            shape((4, S, D), F32), shape((4, S, D), BF16), shape((4, S, D), BF16),
            shape((3, S, D), BF16), shape((2, S, D), BF16), shape((3, S, D), BF16),
        ]
        dma = pltpu.SemaphoreType.DMA
        out = pl.pallas_call(
            kernel,
            out_shape=outs,
            in_specs=[any_] * 7,
            out_specs=[any_] * len(outs),
            scratch_shapes=[
                pltpu.VMEM((S, D), BF16), pltpu.VMEM((S, F), BF16), pltpu.VMEM((S, F), BF16),
                pltpu.VMEM((C, D), F32), pltpu.VMEM((C, D), BF16), pltpu.VMEM((C, D), BF16),
                pltpu.VMEM((C, D), BF16), pltpu.VMEM((C, D), BF16), pltpu.VMEM((C, D), F32),
                dma((2, 2, H)), dma((2, 3, H)), dma((2, 3, H)), dma((2, H)),
                dma((2, 4)), dma((2, 4)), dma((4,)), dma((4,)),
                dma((3, H)), dma((3, H)), dma((2, H)), dma((2, H)), dma((H,)), dma((H,)),
                dma((4,)),
            ],
            compiler_params=pltpu.CompilerParams(
                collective_id=0, has_side_effects=True, vmem_limit_bytes=60 * 2**20),
            name="mlp_backward",
        )(x, dy, gate, up, w_gate, w_up, w_down)
        base, dwg, dwu, dwd, early, last = out[:6]
        last = lax.ppermute(last, "tp", [(2, 0), (3, 1), (4, 6), (5, 7)])
        dx, *grads = finish(base, early, dwg, dwu, dwd)
        done = S - C
        dx = lax.dynamic_update_slice(dx, (base[done:] + last.astype(F32)).astype(BF16), (done, 0))
        return dx, *grads

    both = P(("dp", "tp"), None)
    cols = P("dp", "tp")
    return jax.shard_map(
        step, mesh=mesh,
        in_specs=(both, both, cols, cols, P(None, "tp"), P(None, "tp"), P("tp", None)),
        out_specs=(both, cols, cols, both), check_vma=False)
```

```python
import functools

import jax
import jax.numpy as jnp
from jax import lax
from jax.experimental import pallas as pl
from jax.experimental.pallas import tpu as pltpu
from jax.sharding import PartitionSpec as P

MESH = pl.DeviceIdType.MESH
F32, BF16 = jnp.float32, jnp.bfloat16
H = 3


def last_rows(S):
    return 16 * round(S / 60)


def act(gate, up):
    return jax.nn.gelu(gate) * up


def dot(a, b, ca, cb):
    return lax.dot_general(a, b, (((ca,), (cb,)), ((), ())), preferred_element_type=F32)


def tile_of(n, cap):
    return max(t for t in range(128, min(n, cap) + 1, 128) if n % t == 0)


MID_M = {0: 0, 1: 1, -1: 2, 2: 3}


def kernel(x_ref, dy_ref, gate_ref, up_ref, wg_ref, wu_ref, wd_ref,
           base_ref, base_last, dwg_ref, dwu_ref, dwd_ref, rw, wlast,
           dyg, xg, dgs, dus, pown, pin, tst, ru, rv, rso,
           xv, gv, uv, pc, tc, rc, sc, oc, fc,
           sF, sE, rF, rE, sP, rP, sT, rT, sU, rU, sV, rV, sW, rW, lsem):
    S, D = x_ref.shape
    F = gate_ref.shape[1]
    C = S // H
    L = last_rows(S)
    B = (S - L) // 2
    tp = lax.axis_index("tp")
    z, c = tp // 2, tp % 2
    way = jnp.where(z < 2, 1, -1)
    is_end = (z == 0) | (z == 3)
    is_mid = (z == 1) | (z == 2)

    def chip(k):
        return z + way * k

    def dev(k):
        return {"tp": 2 * chip(k) + c}

    partner = {"tp": 2 * z + 1 - c}
    rows = lambda h: pl.ds(h * C, C)
    wrows = lambda i: pl.ds(i * B, B)
    given, gathered = (dy_ref, x_ref), (dyg, xg)

    def rcopy(src, dst, ssem, rsem, to):
        return pltpu.make_async_remote_copy(
            src_ref=src, dst_ref=dst, send_sem=ssem, recv_sem=rsem, device_id=to, device_id_type=MESH)

    def local(*copies):
        made = [pltpu.make_async_copy(s, d, lsem.at[i]) for i, (s, d) in enumerate(copies)]
        for cp in made:
            cp.start()
        for cp in made:
            cp.wait()

    def piece(a, k, h):
        return gathered[a].at[2 * chip(k) + c, rows(h)]

    def source(a, k, h):
        return given[a].at[rows(h)] if k == 0 else piece(a, k, h)

    def end_to_f(a, h):
        return rcopy(source(a, 0, h), piece(a, 0, h), sF.at[a, 0, h], rE.at[a, h], dev(1))

    def mid_to_f(a, k, h):
        j = 0 if k == 0 else 1
        return rcopy(source(a, k, h), piece(a, k, h), sF.at[a, j, h], rF.at[a, j, h], dev(1))

    def mid_to_e(a, k, h):
        return rcopy(source(a, k, h), piece(a, k, h), sE.at[a, k, h], rF.at[a, k, h], dev(-1))

    def to_partner(a, k, m):
        src = given[a] if k == 0 else gathered[a].at[2 * chip(k) + c]
        return rcopy(src, gathered[a].at[2 * chip(k) + c], sP.at[a, m], rP.at[a, m], partner)

    def wait_f(a, k, h):
        rcopy(piece(a, k, h), piece(a, k, h), sF.at[a, 0, h], rF.at[a, k - 1, h], partner).wait_recv()

    def wait_e(a, h):
        rcopy(piece(a, -1, h), piece(a, -1, h), sF.at[a, 0, h], rE.at[a, h], partner).wait_recv()

    def term(m):
        return rcopy(tst.at[m], pin.at[m], sT.at[m], rT.at[m], partner)

    def u_copy(j, h):
        return rcopy(rso.at[j, rows(h)], ru.at[j, rows(h)], sU.at[j, h], rU.at[j, h], dev(1))

    def v_copy(j, h):
        return rcopy(rso.at[j, rows(h)], rv.at[j, rows(h)], sV.at[j, h], rV.at[j, h], dev(1))

    def w_copy(i):
        return rcopy(rso.at[2, wrows(i)], rw.at[wrows(i)], sW.at[i], rW.at[i], dev(-1))

    def combine(m, at, received, out, res=oc):
        n = at.size
        bufs = [b.at[pl.ds(0, n)] for b in (pc, tc, rc, sc)]
        res = res.at[pl.ds(0, n)]
        srcs = [pown.at[m, at], pin.at[m, at], *received]
        local(*zip(srcs, bufs))
        step = 16

        @pl.loop(0, n // step)
        def _(i):
            r = pl.ds(pl.multiple_of(i * step, step), step)
            total = bufs[0][r, :]
            for b in bufs[1:len(srcs)]:
                total += b[r, :].astype(F32)
            res[r, :] = total.astype(res.dtype)

        local((res, out))

    barrier = pltpu.get_barrier_semaphore()
    pl.semaphore_signal(barrier, inc=1, device_id=partner, device_id_type=MESH)
    pl.semaphore_signal(barrier, inc=1, device_id=dev(1), device_id_type=MESH)

    @pl.when(is_mid)
    def _():
        pl.semaphore_signal(barrier, inc=1, device_id=dev(-1), device_id_type=MESH)
        pl.semaphore_wait(barrier, 3)

    @pl.when(is_end)
    def _():
        pl.semaphore_wait(barrier, 2)

    @pl.when(is_mid)
    def _():
        for h in range(H):
            mid_to_e(0, 0, h).start()
            mid_to_f(0, 0, h).start()

    @pl.when(is_end)
    def _():
        for h in range(H):
            end_to_f(0, h).start()
        for h in range(H):
            end_to_f(1, h).start()

    for a in range(2):
        to_partner(a, 0, 0).start()

    def k_of(m):
        mid = jnp.where(m == 2, -1, jnp.where(m == 3, 2, m))
        return jnp.where(is_end, m, mid)

    def load_shard(a, m, p):
        t = 2 * (z + way * k_of(m)) + jnp.where(p == 0, c, 1 - c)

        @pl.when(p == 1)
        def _():
            rcopy(gathered[a].at[t], gathered[a].at[t], sP.at[a, m], rP.at[a, m], partner).wait_recv()

        @pl.when((m == 0) & (p == 0))
        def _():
            pltpu.make_async_copy(given[a], xv, lsem.at[2]).start()

        @pl.when((m > 0) | (p > 0))
        def _():
            pltpu.make_async_copy(gathered[a].at[t], xv, lsem.at[2]).start()

        return t

    def phase1(wd, wg, wu, accd, hid, dgv, duv, dxf, dxb, stage):
        local((wd_ref, wd), (wg_ref, wg))
        local((wu_ref, wu))
        accd[...] = jnp.zeros_like(accd)

        def unit(m, p):
            t = load_shard(0, m, p)
            local((gate_ref.at[pl.ds(t * S, S)], gv), (up_ref.at[pl.ds(t * S, S)], uv))
            pltpu.make_async_copy(given[0], xv, lsem.at[2]).wait()
            tn = min(F, 256)

            @pl.loop(0, pl.cdiv(F, tn))
            def _(n):
                s = pl.ds(pl.multiple_of(jnp.minimum(n * tn, F - tn), 128), tn)
                d_hidden = dot(xv[...], wd[s, :], 1, 1)
                hidden, back = jax.vjp(act, gv[:, s].astype(F32), uv[:, s].astype(F32))
                d_gate, d_up = back(d_hidden)
                hid[:, s] = hidden.astype(BF16)
                dgv[:, s] = d_gate.astype(BF16)
                duv[:, s] = d_up.astype(BF16)

            keep = [pltpu.make_async_copy(v, o.at[2 * m + p], lsem.at[i])
                    for i, (v, o) in enumerate(((dgv, dgs), (duv, dus)))]
            for cp in keep:
                cp.start()
            tn2 = tile_of(D, 256)

            @pl.loop(0, D // tn2)
            def _(n):
                s = pl.ds(pl.multiple_of(n * tn2, tn2), tn2)
                part = dot(dgv[...], wg[s, :], 1, 1) + dot(duv[...], wu[s, :], 1, 1)
                dxf[:, s] = part
                dxb[:, s] = part.astype(BF16)

            for cp in keep:
                cp.wait()

            @pl.when(p == 0)
            def _():
                local((dxf, pown.at[m]))

            @pl.when(p == 1)
            def _():
                local((dxb, tst.at[m]))
                term(m).start()

            tn3 = tile_of(D, 768)

            @pl.loop(0, D // tn3)
            def _(n):
                s = pl.ds(pl.multiple_of(n * tn3, tn3), tn3)
                accd[:, s] += dot(hid[...], xv[:, s], 0, 0)

        def wait_term(m):
            term(m).wait_recv()

        def send_u(j):
            wait_term(j + 1)
            for h in range(H):
                combine(j + 1, rows(h), [], rso.at[j, rows(h)])
                u_copy(j, h).start()

        @pl.loop(0, 4)
        def _(m):
            @pl.loop(0, 2)
            def _(p):
                unit(m, p)

            @pl.when((m == 0) & is_end)
            def _():
                for h in range(H):
                    wait_f(0, 1, h)
                to_partner(0, 1, 1).start()

            @pl.when((m == 0) & is_mid)
            def _():
                for h in range(H):
                    wait_f(0, 1, h)
                    mid_to_e(0, 1, h).start()
                    wait_e(0, h)
                    mid_to_f(0, -1, h).start()
                to_partner(0, 1, 1).start()
                to_partner(0, -1, 2).start()
                for h in range(H):
                    mid_to_f(1, 0, h).start()

            @pl.when((m == 1) & is_end)
            def _():
                send_u(0)
                for h in range(H):
                    wait_f(0, 2, h)
                to_partner(0, 2, 2).start()

            @pl.when((m == 1) & is_mid)
            def _():
                for h in range(H):
                    wait_f(0, 2, h)
                    mid_to_e(0, 2, h).start()
                to_partner(0, 2, 3).start()
                for h in range(H):
                    mid_to_e(1, 0, h).start()
                for h in range(H):
                    wait_e(1, h)
                    mid_to_f(1, -1, h).start()
                to_partner(1, -1, 2).start()

            @pl.when((m == 2) & is_end)
            def _():
                send_u(1)
                for h in range(H):
                    wait_f(0, 3, h)
                to_partner(0, 3, 3).start()

            @pl.when((m == 2) & is_mid)
            def _():
                for h in range(H):
                    wait_f(1, 1, h)
                    mid_to_e(1, 1, h).start()
                to_partner(1, 1, 1).start()

            @pl.when((m == 3) & is_end)
            def _():
                send_u(2)

        flush([(accd, dwd_ref)], stage)

    def flush(pairs, stage):
        n = stage.shape[1]
        jobs = [(acc, out, r) for acc, out in pairs for r in range(0, acc.shape[0], n)]
        made = []
        for i, (acc, out, r) in enumerate(jobs):
            if i >= 2:
                made[i - 2].wait()
            stage[i % 2] = acc[r:r + n, :].astype(BF16)
            made.append(pltpu.make_async_copy(stage.at[i % 2], out.at[pl.ds(r, n)], lsem.at[i % 2]))
            made[i].start()
        for cp in made[-2:]:
            cp.wait()

    def own_rows():
        term(0).wait_recv()
        parts = [(wrows(0), base_ref.at[wrows(0)]), (wrows(1), base_ref.at[wrows(1)]), (pl.ds(S - L, L), base_last)]

        @pl.when(is_mid)
        def _():
            for h in range(H):
                rcopy(ru.at[0, rows(h)], ru.at[0, rows(h)], sU.at[0, h], rU.at[0, h], partner).wait_recv()
                rcopy(rv.at[0, rows(h)], rv.at[0, rows(h)], sV.at[0, h], rV.at[0, h], partner).wait_recv()
            for at, out in parts:
                combine(0, at, [ru.at[0, at], rv.at[0, at]], out, fc)

        @pl.when(is_end)
        def _():
            for at, out in parts:
                combine(0, at, [], out, fc)

    def send_v(j):
        m = MID_M[j + 1]
        term(m).wait_recv()
        for h in range(H):
            rcopy(ru.at[j + 1, rows(h)], ru.at[j + 1, rows(h)], sU.at[j + 1, h], rU.at[j + 1, h], partner).wait_recv()
            combine(m, rows(h), [ru.at[j + 1, rows(h)]], rso.at[j, rows(h)])
            v_copy(j, h).start()

    def send_w():
        m = MID_M[-1]
        term(m).wait_recv()
        came = lambda h: rcopy(
            rv.at[1, rows(h)], rv.at[1, rows(h)], sV.at[1, h], rV.at[1, h], partner).wait_recv()
        came(0)
        came(1)
        combine(m, wrows(0), [rv.at[1, wrows(0)]], rso.at[2, wrows(0)])
        w_copy(0).start()
        came(2)
        combine(m, wrows(1), [rv.at[1, wrows(1)]], rso.at[2, wrows(1)])
        w_copy(1).start()
        at = pl.ds(S - L, L)
        combine(m, at, [rv.at[1, at]], wlast)

    def phase2(accg, accu, stage):
        accg[...] = jnp.zeros_like(accg)
        accu[...] = jnp.zeros_like(accu)

        def unit(m, p):
            load_shard(1, m, p)
            local((dgs.at[2 * m + p], gv), (dus.at[2 * m + p], uv))
            pltpu.make_async_copy(given[1], xv, lsem.at[2]).wait()
            tm = tile_of(D, 768)

            @pl.loop(0, D // tm)
            def _(n):
                s = pl.ds(pl.multiple_of(n * tm, tm), tm)
                accg[s, :] += dot(xv[:, s], gv[...], 0, 0)
                accu[s, :] += dot(xv[:, s], uv[...], 0, 0)

        @pl.loop(0, 4)
        def _(m):
            @pl.when((m == 0) & is_mid)
            def _():
                send_v(0)

            @pl.when((m == 1) & is_mid)
            def _():
                for h in range(H):
                    wait_f(1, 2, h)
                    mid_to_e(1, 2, h).start()
                to_partner(1, 2, 3).start()

            @pl.when((m == 2) & is_mid)
            def _():
                send_v(1)

            @pl.when((m == 3) & is_end)
            def _():
                own_rows()

            for i in range(1, 4):
                @pl.when((m == i) & is_end)
                def _(i=i):
                    for h in range(H):
                        wait_f(1, i, h)
                    to_partner(1, i, i).start()

            @pl.loop(0, 2)
            def _(p):
                unit(m, p)

        @pl.when(is_mid)
        def _():
            send_w()
            own_rows()

        flush([(accg, dwg_ref), (accu, dwu_ref)], stage)

    wbuf = lambda r: pltpu.VMEM(r.shape, r.dtype)
    pl.run_scoped(
        phase1, wbuf(wd_ref), wbuf(wg_ref), wbuf(wu_ref), pltpu.VMEM((F, D), F32),
        pltpu.VMEM((S, F), BF16), pltpu.VMEM((S, F), BF16), pltpu.VMEM((S, F), BF16),
        pltpu.VMEM((S, D), F32), pltpu.VMEM((S, D), BF16), pltpu.VMEM((2, tile_of(F, 128), D), BF16))
    pl.run_scoped(
        phase2, pltpu.VMEM((D, F), F32), pltpu.VMEM((D, F), F32), pltpu.VMEM((2, tile_of(D, 256), F), BF16))

    for m in range(4):
        term(m).wait_send()

    @pl.when(is_end)
    def _():
        for a in range(2):
            for h in range(H):
                end_to_f(a, h).wait_send()
            for k in range(4):
                to_partner(a, k, k).wait_send()
        for j in range(3):
            for h in range(H):
                u_copy(j, h).wait_send()
        for i in range(2):
            rcopy(rw.at[wrows(i)], rw.at[wrows(i)], sW.at[i], rW.at[i], partner).wait_recv()

    @pl.when(is_mid)
    def _():
        for a in range(2):
            for h in range(H):
                for k in (0, 1, 2):
                    mid_to_e(a, k, h).wait_send()
                for k in (0, -1):
                    mid_to_f(a, k, h).wait_send()
            for k, m in MID_M.items():
                to_partner(a, k, m).wait_send()
        for h in range(H):
            for j in range(2):
                v_copy(j, h).wait_send()
        for i in range(2):
            w_copy(i).wait_send()


def finish_kernel(base, part, gate_in, up_in, down_in, dx, gate_out, up_out, down_out, gv, uv, dv, bv, pv, ov, isem, osem):
    n = part.shape[0]
    bring = [pltpu.make_async_copy(base, bv, isem.at[0]), pltpu.make_async_copy(part, pv, isem.at[1])]
    put = []
    for src, v, dst in ((gate_in, gv, gate_out), (up_in, uv, up_out), (down_in, dv, down_out)):
        size = src.shape[0] // 3
        for r in range(3):
            piece = pl.ds(r * size, size)
            bring.append(pltpu.make_async_copy(src.at[piece], v.at[piece], isem.at[len(bring)]))
            put.append(pltpu.make_async_copy(v.at[piece], dst.at[piece], osem.at[len(put)]))
    for cp in bring:
        cp.start()
    bring[0].wait()
    bring[1].wait()
    tp = lax.axis_index("tp")
    is_end = (tp < 2) | (tp >= 6)
    step = 16

    @pl.loop(0, n // step)
    def _(i):
        r = pl.ds(pl.multiple_of(i * step, step), step)
        ov[r, :] = (bv[r, :] + jnp.where(is_end, pv[r, :].astype(F32), 0.0)).astype(BF16)

    put.append(pltpu.make_async_copy(ov, dx.at[pl.ds(0, n)], osem.at[len(put)]))
    put[-1].start()
    for got, cp in zip(bring[2:], put):
        got.wait()
        cp.start()
    for cp in put:
        cp.wait()


def finish(S, base, part, *grads):
    n, D = base.shape
    any_ = pl.BlockSpec(memory_space=pl.ANY)
    moved = 2 * sum(g.size * 2 for g in grads)
    return pl.pallas_call(
        finish_kernel, in_specs=[any_] * 5, out_specs=[any_] * 4,
        out_shape=[jax.ShapeDtypeStruct((S, D), BF16)] + [jax.ShapeDtypeStruct(g.shape, BF16) for g in grads],
        scratch_shapes=[pltpu.VMEM(g.shape, BF16) for g in grads] + [
            pltpu.VMEM((n, D), F32), pltpu.VMEM((n, D), BF16), pltpu.VMEM((n, D), BF16),
            pltpu.SemaphoreType.DMA((11,)), pltpu.SemaphoreType.DMA((10,))],
        compiler_params=pltpu.CompilerParams(vmem_limit_bytes=62 * 2**20),
        cost_estimate=pl.CostEstimate(flops=10**9, bytes_accessed=moved, transcendentals=0),
        name="finish")(base, part, *grads)


def solution(mesh):
    def step(x, dy, gate, up, w_gate, w_up, w_down):
        (S, D), F = x.shape, gate.shape[1]
        L = last_rows(S)
        B = (S - L) // 2
        shape = jax.ShapeDtypeStruct
        any_ = pl.BlockSpec(memory_space=pl.ANY)
        outs = [
            shape((S - L, D), F32), shape((L, D), F32),
            shape((D, F), BF16), shape((D, F), BF16), shape((F, D), BF16),
            shape((S - L, D), BF16), shape((L, D), BF16),
            shape((8, S, D), BF16), shape((8, S, D), BF16),
            shape((8, S, F), BF16), shape((8, S, F), BF16),
            shape((4, S, D), F32), shape((4, S, D), BF16), shape((4, S, D), BF16),
            shape((3, S, D), BF16), shape((2, S, D), BF16), shape((3, S, D), BF16),
        ]
        dma = pltpu.SemaphoreType.DMA
        out = pl.pallas_call(
            kernel,
            out_shape=outs,
            in_specs=[any_] * 7,
            out_specs=[any_] * len(outs),
            scratch_shapes=[
                pltpu.VMEM((S, D), BF16), pltpu.VMEM((S, F), BF16), pltpu.VMEM((S, F), BF16),
                pltpu.VMEM((B, D), F32), pltpu.VMEM((B, D), BF16), pltpu.VMEM((B, D), BF16),
                pltpu.VMEM((B, D), BF16), pltpu.VMEM((B, D), BF16), pltpu.VMEM((B, D), F32),
                dma((2, 2, H)), dma((2, 3, H)), dma((2, 3, H)), dma((2, H)),
                dma((2, 4)), dma((2, 4)), dma((4,)), dma((4,)),
                dma((3, H)), dma((3, H)), dma((2, H)), dma((2, H)), dma((2,)), dma((2,)),
                dma((4,)),
            ],
            compiler_params=pltpu.CompilerParams(
                collective_id=0, has_side_effects=True, vmem_limit_bytes=60 * 2**20),
            name="mlp_backward",
        )(x, dy, gate, up, w_gate, w_up, w_down)
        base, base_last, dwg, dwu, dwd, early, last = out[:7]
        last = lax.ppermute(last, "tp", [(2, 0), (3, 1), (4, 6), (5, 7)])
        dx, *grads = finish(S, base, early, dwg, dwu, dwd)
        last = (base_last + last.astype(F32)).astype(BF16)
        return lax.dynamic_update_slice(dx, last, (S - L, 0)), *grads

    both = P(("dp", "tp"), None)
    cols = P("dp", "tp")
    return jax.shard_map(
        step, mesh=mesh,
        in_specs=(both, both, cols, cols, P(None, "tp"), P(None, "tp"), P("tp", None)),
        out_specs=(both, cols, cols, both), check_vma=False)
```

```python
import functools

import jax
import jax.numpy as jnp
from jax import lax
from jax.experimental import pallas as pl
from jax.experimental.pallas import tpu as pltpu
from jax.sharding import PartitionSpec as P

MESH = pl.DeviceIdType.MESH
F32, BF16 = jnp.float32, jnp.bfloat16
H = 3


def last_rows(S):
    return 16 * round(S / 48)


def act(gate, up):
    return jax.nn.gelu(gate) * up


def dot(a, b, ca, cb):
    return lax.dot_general(a, b, (((ca,), (cb,)), ((), ())), preferred_element_type=F32)


def tile_of(n, cap):
    return max(t for t in range(128, min(n, cap) + 1, 128) if n % t == 0)


MID_M = {0: 0, 1: 1, -1: 2, 2: 3}


def kernel(x_ref, dy_ref, gate_ref, up_ref, wg_ref, wu_ref, wd_ref,
           base_ref, base_last, dwg_ref, dwu_ref, dwd_ref, rw, wlast,
           dyg, xg, dgs, dus, pown, pin, tst, ru, rv, rso,
           xv, gv, uv, pc, tc, rc, sc, oc, fc,
           sF, sE, rF, rE, sP, rP, sT, rT, sU, rU, sV, rV, sW, rW, lsem):
    S, D = x_ref.shape
    F = gate_ref.shape[1]
    C = S // H
    L = last_rows(S)
    B = (S - L) // 2
    tp = lax.axis_index("tp")
    z, c = tp // 2, tp % 2
    way = jnp.where(z < 2, 1, -1)
    is_end = (z == 0) | (z == 3)
    is_mid = (z == 1) | (z == 2)

    def chip(k):
        return z + way * k

    def dev(k):
        return {"tp": 2 * chip(k) + c}

    partner = {"tp": 2 * z + 1 - c}
    rows = lambda h: pl.ds(h * C, C)
    wrows = lambda i: pl.ds(i * B, B)
    given, gathered = (dy_ref, x_ref), (dyg, xg)

    def rcopy(src, dst, ssem, rsem, to):
        return pltpu.make_async_remote_copy(
            src_ref=src, dst_ref=dst, send_sem=ssem, recv_sem=rsem, device_id=to, device_id_type=MESH)

    def local(*copies):
        made = [pltpu.make_async_copy(s, d, lsem.at[i]) for i, (s, d) in enumerate(copies)]
        for cp in made:
            cp.start()
        for cp in made:
            cp.wait()

    def piece(a, k, h):
        return gathered[a].at[2 * chip(k) + c, rows(h)]

    def source(a, k, h):
        return given[a].at[rows(h)] if k == 0 else piece(a, k, h)

    def end_to_f(a, h):
        return rcopy(source(a, 0, h), piece(a, 0, h), sF.at[a, 0, h], rE.at[a, h], dev(1))

    def mid_to_f(a, k, h):
        j = 0 if k == 0 else 1
        return rcopy(source(a, k, h), piece(a, k, h), sF.at[a, j, h], rF.at[a, j, h], dev(1))

    def mid_to_e(a, k, h):
        return rcopy(source(a, k, h), piece(a, k, h), sE.at[a, k, h], rF.at[a, k, h], dev(-1))

    def to_partner(a, k, m):
        src = given[a] if k == 0 else gathered[a].at[2 * chip(k) + c]
        return rcopy(src, gathered[a].at[2 * chip(k) + c], sP.at[a, m], rP.at[a, m], partner)

    def wait_f(a, k, h):
        rcopy(piece(a, k, h), piece(a, k, h), sF.at[a, 0, h], rF.at[a, k - 1, h], partner).wait_recv()

    def wait_e(a, h):
        rcopy(piece(a, -1, h), piece(a, -1, h), sF.at[a, 0, h], rE.at[a, h], partner).wait_recv()

    def term(m):
        return rcopy(tst.at[m], pin.at[m], sT.at[m], rT.at[m], partner)

    def u_copy(j, h):
        return rcopy(rso.at[j, rows(h)], ru.at[j, rows(h)], sU.at[j, h], rU.at[j, h], dev(1))

    def v_copy(j, h):
        return rcopy(rso.at[j, rows(h)], rv.at[j, rows(h)], sV.at[j, h], rV.at[j, h], dev(1))

    def w_copy(i):
        return rcopy(rso.at[2, wrows(i)], rw.at[wrows(i)], sW.at[i], rW.at[i], dev(-1))

    def combine(m, at, received, out, res=oc):
        n = at.size
        bufs = [b.at[pl.ds(0, n)] for b in (pc, tc, rc, sc)]
        res = res.at[pl.ds(0, n)]
        srcs = [pown.at[m, at], pin.at[m, at], *received]
        local(*zip(srcs, bufs))
        step = 16

        @pl.loop(0, n // step)
        def _(i):
            r = pl.ds(pl.multiple_of(i * step, step), step)
            total = bufs[0][r, :]
            for b in bufs[1:len(srcs)]:
                total += b[r, :].astype(F32)
            res[r, :] = total.astype(res.dtype)

        local((res, out))

    barrier = pltpu.get_barrier_semaphore()
    pl.semaphore_signal(barrier, inc=1, device_id=partner, device_id_type=MESH)
    pl.semaphore_signal(barrier, inc=1, device_id=dev(1), device_id_type=MESH)

    @pl.when(is_mid)
    def _():
        pl.semaphore_signal(barrier, inc=1, device_id=dev(-1), device_id_type=MESH)
        pl.semaphore_wait(barrier, 3)

    @pl.when(is_end)
    def _():
        pl.semaphore_wait(barrier, 2)

    def first_sends(core):
        @pl.when(is_mid & (c == core))
        def _():
            for h in range(H):
                mid_to_e(0, 0, h).start()
                mid_to_f(0, 0, h).start()

        @pl.when(is_end & (c == core))
        def _():
            for h in range(H):
                end_to_f(0, h).start()
            for h in range(H):
                end_to_f(1, h).start()

    first_sends(1)

    for a in range(2):
        to_partner(a, 0, 0).start()

    def k_of(m):
        mid = jnp.where(m == 2, -1, jnp.where(m == 3, 2, m))
        return jnp.where(is_end, m, mid)

    def load_shard(a, m, p):
        t = 2 * (z + way * k_of(m)) + jnp.where(p == 0, c, 1 - c)

        @pl.when(p == 1)
        def _():
            rcopy(gathered[a].at[t], gathered[a].at[t], sP.at[a, m], rP.at[a, m], partner).wait_recv()

        @pl.when((m == 0) & (p == 0))
        def _():
            pltpu.make_async_copy(given[a], xv, lsem.at[2]).start()

        @pl.when((m > 0) | (p > 0))
        def _():
            pltpu.make_async_copy(gathered[a].at[t], xv, lsem.at[2]).start()

        return t

    def phase1(wd, wg, wu, accd, hid, dgv, duv, dxf, dxb, stage):
        local((wd_ref, wd))
        first_sends(0)
        local((wg_ref, wg), (wu_ref, wu))
        accd[...] = jnp.zeros_like(accd)

        def unit(m, p):
            t = load_shard(0, m, p)
            local((gate_ref.at[pl.ds(t * S, S)], gv), (up_ref.at[pl.ds(t * S, S)], uv))
            pltpu.make_async_copy(given[0], xv, lsem.at[2]).wait()
            tn = min(F, 256)

            @pl.loop(0, pl.cdiv(F, tn))
            def _(n):
                s = pl.ds(pl.multiple_of(jnp.minimum(n * tn, F - tn), 128), tn)
                d_hidden = dot(xv[...], wd[s, :], 1, 1)
                hidden, back = jax.vjp(act, gv[:, s].astype(F32), uv[:, s].astype(F32))
                d_gate, d_up = back(d_hidden)
                hid[:, s] = hidden.astype(BF16)
                dgv[:, s] = d_gate.astype(BF16)
                duv[:, s] = d_up.astype(BF16)

            keep = [pltpu.make_async_copy(v, o.at[2 * m + p], lsem.at[i])
                    for i, (v, o) in enumerate(((dgv, dgs), (duv, dus)))]
            for cp in keep:
                cp.start()
            tn2 = tile_of(D, 256)

            @pl.loop(0, D // tn2)
            def _(n):
                s = pl.ds(pl.multiple_of(n * tn2, tn2), tn2)
                part = dot(dgv[...], wg[s, :], 1, 1) + dot(duv[...], wu[s, :], 1, 1)
                dxf[:, s] = part
                dxb[:, s] = part.astype(BF16)

            for cp in keep:
                cp.wait()

            @pl.when(p == 0)
            def _():
                local((dxf, pown.at[m]))

            @pl.when(p == 1)
            def _():
                local((dxb, tst.at[m]))
                term(m).start()

            tn3 = tile_of(D, 768)

            @pl.loop(0, D // tn3)
            def _(n):
                s = pl.ds(pl.multiple_of(n * tn3, tn3), tn3)
                accd[:, s] += dot(hid[...], xv[:, s], 0, 0)

        def wait_term(m):
            term(m).wait_recv()

        def send_u(j):
            wait_term(j + 1)
            for h in range(H):
                combine(j + 1, rows(h), [], rso.at[j, rows(h)])
                u_copy(j, h).start()

        @pl.loop(0, 4)
        def _(m):
            @pl.loop(0, 2)
            def _(p):
                unit(m, p)

            @pl.when((m == 0) & is_end)
            def _():
                for h in range(H):
                    wait_f(0, 1, h)
                to_partner(0, 1, 1).start()

            @pl.when((m == 0) & is_mid)
            def _():
                for h in range(H):
                    wait_f(0, 1, h)
                    mid_to_e(0, 1, h).start()
                    wait_e(0, h)
                    mid_to_f(0, -1, h).start()
                to_partner(0, 1, 1).start()
                to_partner(0, -1, 2).start()
                for h in range(H):
                    mid_to_f(1, 0, h).start()

            @pl.when((m == 1) & is_end)
            def _():
                send_u(0)
                for h in range(H):
                    wait_f(0, 2, h)
                to_partner(0, 2, 2).start()

            @pl.when((m == 1) & is_mid)
            def _():
                for h in range(H):
                    wait_f(0, 2, h)
                    mid_to_e(0, 2, h).start()
                to_partner(0, 2, 3).start()
                for h in range(H):
                    mid_to_e(1, 0, h).start()
                for h in range(H):
                    wait_e(1, h)
                    mid_to_f(1, -1, h).start()
                to_partner(1, -1, 2).start()

            @pl.when((m == 2) & is_end)
            def _():
                send_u(1)
                for h in range(H):
                    wait_f(0, 3, h)
                to_partner(0, 3, 3).start()

            @pl.when((m == 2) & is_mid)
            def _():
                for h in range(H):
                    wait_f(1, 1, h)
                    mid_to_e(1, 1, h).start()
                to_partner(1, 1, 1).start()

            @pl.when((m == 3) & is_end)
            def _():
                send_u(2)

        flush([(accd, dwd_ref)], stage)

    def flush(pairs, stage):
        n = stage.shape[1]
        jobs = [(acc, out, r) for acc, out in pairs for r in range(0, acc.shape[0], n)]
        made = []
        for i, (acc, out, r) in enumerate(jobs):
            if i >= 2:
                made[i - 2].wait()
            stage[i % 2] = acc[r:r + n, :].astype(BF16)
            made.append(pltpu.make_async_copy(stage.at[i % 2], out.at[pl.ds(r, n)], lsem.at[i % 2]))
            made[i].start()
        for cp in made[-2:]:
            cp.wait()

    def own_rows():
        term(0).wait_recv()
        parts = [(wrows(0), base_ref.at[wrows(0)]), (wrows(1), base_ref.at[wrows(1)]), (pl.ds(S - L, L), base_last)]

        @pl.when(is_mid)
        def _():
            for h in range(H):
                rcopy(ru.at[0, rows(h)], ru.at[0, rows(h)], sU.at[0, h], rU.at[0, h], partner).wait_recv()
                rcopy(rv.at[0, rows(h)], rv.at[0, rows(h)], sV.at[0, h], rV.at[0, h], partner).wait_recv()
            for at, out in parts:
                combine(0, at, [ru.at[0, at], rv.at[0, at]], out, fc)

        @pl.when(is_end)
        def _():
            for at, out in parts:
                combine(0, at, [], out, fc)

    def send_v(j):
        m = MID_M[j + 1]
        term(m).wait_recv()
        for h in range(H):
            rcopy(ru.at[j + 1, rows(h)], ru.at[j + 1, rows(h)], sU.at[j + 1, h], rU.at[j + 1, h], partner).wait_recv()
            combine(m, rows(h), [ru.at[j + 1, rows(h)]], rso.at[j, rows(h)])
            v_copy(j, h).start()

    def send_w():
        m = MID_M[-1]
        term(m).wait_recv()
        came = lambda h: rcopy(
            rv.at[1, rows(h)], rv.at[1, rows(h)], sV.at[1, h], rV.at[1, h], partner).wait_recv()
        came(0)
        came(1)
        combine(m, wrows(0), [rv.at[1, wrows(0)]], rso.at[2, wrows(0)])
        w_copy(0).start()
        came(2)
        combine(m, wrows(1), [rv.at[1, wrows(1)]], rso.at[2, wrows(1)])
        w_copy(1).start()
        at = pl.ds(S - L, L)
        combine(m, at, [rv.at[1, at]], wlast)

    def phase2(accg, accu, stage):
        accg[...] = jnp.zeros_like(accg)
        accu[...] = jnp.zeros_like(accu)

        def unit(m, p):
            load_shard(1, m, p)
            local((dgs.at[2 * m + p], gv), (dus.at[2 * m + p], uv))
            pltpu.make_async_copy(given[1], xv, lsem.at[2]).wait()
            tm = tile_of(D, 768)

            @pl.loop(0, D // tm)
            def _(n):
                s = pl.ds(pl.multiple_of(n * tm, tm), tm)
                accg[s, :] += dot(xv[:, s], gv[...], 0, 0)
                accu[s, :] += dot(xv[:, s], uv[...], 0, 0)

        @pl.loop(0, 4)
        def _(m):
            @pl.when((m == 0) & is_mid)
            def _():
                send_v(0)

            @pl.when((m == 1) & is_mid)
            def _():
                for h in range(H):
                    wait_f(1, 2, h)
                    mid_to_e(1, 2, h).start()
                to_partner(1, 2, 3).start()

            @pl.when((m == 2) & is_mid)
            def _():
                send_v(1)

            @pl.when((m == 3) & is_end)
            def _():
                own_rows()

            for i in range(1, 4):
                @pl.when((m == i) & is_end)
                def _(i=i):
                    for h in range(H):
                        wait_f(1, i, h)
                    to_partner(1, i, i).start()

            @pl.loop(0, 2)
            def _(p):
                unit(m, p)

        @pl.when(is_mid)
        def _():
            send_w()
            own_rows()

        flush([(accg, dwg_ref), (accu, dwu_ref)], stage)

    wbuf = lambda r: pltpu.VMEM(r.shape, r.dtype)
    pl.run_scoped(
        phase1, wbuf(wd_ref), wbuf(wg_ref), wbuf(wu_ref), pltpu.VMEM((F, D), F32),
        pltpu.VMEM((S, F), BF16), pltpu.VMEM((S, F), BF16), pltpu.VMEM((S, F), BF16),
        pltpu.VMEM((S, D), F32), pltpu.VMEM((S, D), BF16), pltpu.VMEM((2, tile_of(F, 128), D), BF16))
    pl.run_scoped(
        phase2, pltpu.VMEM((D, F), F32), pltpu.VMEM((D, F), F32), pltpu.VMEM((2, tile_of(D, 256), F), BF16))

    for m in range(4):
        term(m).wait_send()

    @pl.when(is_end)
    def _():
        for a in range(2):
            for h in range(H):
                end_to_f(a, h).wait_send()
            for k in range(4):
                to_partner(a, k, k).wait_send()
        for j in range(3):
            for h in range(H):
                u_copy(j, h).wait_send()
        for i in range(2):
            rcopy(rw.at[wrows(i)], rw.at[wrows(i)], sW.at[i], rW.at[i], partner).wait_recv()

    @pl.when(is_mid)
    def _():
        for a in range(2):
            for h in range(H):
                for k in (0, 1, 2):
                    mid_to_e(a, k, h).wait_send()
                for k in (0, -1):
                    mid_to_f(a, k, h).wait_send()
            for k, m in MID_M.items():
                to_partner(a, k, m).wait_send()
        for h in range(H):
            for j in range(2):
                v_copy(j, h).wait_send()
        for i in range(2):
            w_copy(i).wait_send()


def finish_kernel(base, part, gate_in, up_in, down_in, dx, gate_out, up_out, down_out, gv, uv, dv, bv, pv, ov, isem, osem):
    n = part.shape[0]
    bring = [pltpu.make_async_copy(base, bv, isem.at[0]), pltpu.make_async_copy(part, pv, isem.at[1])]
    put = []
    for src, v, dst in ((gate_in, gv, gate_out), (up_in, uv, up_out), (down_in, dv, down_out)):
        size = src.shape[0] // 3
        for r in range(3):
            piece = pl.ds(r * size, size)
            bring.append(pltpu.make_async_copy(src.at[piece], v.at[piece], isem.at[len(bring)]))
            put.append(pltpu.make_async_copy(v.at[piece], dst.at[piece], osem.at[len(put)]))
    for cp in bring:
        cp.start()
    bring[0].wait()
    bring[1].wait()
    tp = lax.axis_index("tp")
    is_end = (tp < 2) | (tp >= 6)
    step = 16

    @pl.loop(0, n // step)
    def _(i):
        r = pl.ds(pl.multiple_of(i * step, step), step)
        ov[r, :] = (bv[r, :] + jnp.where(is_end, pv[r, :].astype(F32), 0.0)).astype(BF16)

    put.append(pltpu.make_async_copy(ov, dx.at[pl.ds(0, n)], osem.at[len(put)]))
    put[-1].start()
    for got, cp in zip(bring[2:], put):
        got.wait()
        cp.start()
    for cp in put:
        cp.wait()


def finish(S, base, part, *grads):
    n, D = base.shape
    any_ = pl.BlockSpec(memory_space=pl.ANY)
    moved = 2 * sum(g.size * 2 for g in grads)
    return pl.pallas_call(
        finish_kernel, in_specs=[any_] * 5, out_specs=[any_] * 4,
        out_shape=[jax.ShapeDtypeStruct((S, D), BF16)] + [jax.ShapeDtypeStruct(g.shape, BF16) for g in grads],
        scratch_shapes=[pltpu.VMEM(g.shape, BF16) for g in grads] + [
            pltpu.VMEM((n, D), F32), pltpu.VMEM((n, D), BF16), pltpu.VMEM((n, D), BF16),
            pltpu.SemaphoreType.DMA((11,)), pltpu.SemaphoreType.DMA((10,))],
        compiler_params=pltpu.CompilerParams(vmem_limit_bytes=62 * 2**20),
        cost_estimate=pl.CostEstimate(flops=10**9, bytes_accessed=moved, transcendentals=0),
        name="finish")(base, part, *grads)


def solution(mesh):
    def step(x, dy, gate, up, w_gate, w_up, w_down):
        (S, D), F = x.shape, gate.shape[1]
        L = last_rows(S)
        B = (S - L) // 2
        shape = jax.ShapeDtypeStruct
        any_ = pl.BlockSpec(memory_space=pl.ANY)
        outs = [
            shape((S - L, D), F32), shape((L, D), F32),
            shape((D, F), BF16), shape((D, F), BF16), shape((F, D), BF16),
            shape((S - L, D), BF16), shape((L, D), BF16),
            shape((8, S, D), BF16), shape((8, S, D), BF16),
            shape((8, S, F), BF16), shape((8, S, F), BF16),
            shape((4, S, D), F32), shape((4, S, D), BF16), shape((4, S, D), BF16),
            shape((3, S, D), BF16), shape((2, S, D), BF16), shape((3, S, D), BF16),
        ]
        dma = pltpu.SemaphoreType.DMA
        out = pl.pallas_call(
            kernel,
            out_shape=outs,
            in_specs=[any_] * 7,
            out_specs=[any_] * len(outs),
            scratch_shapes=[
                pltpu.VMEM((S, D), BF16), pltpu.VMEM((S, F), BF16), pltpu.VMEM((S, F), BF16),
                pltpu.VMEM((B, D), F32), pltpu.VMEM((B, D), BF16), pltpu.VMEM((B, D), BF16),
                pltpu.VMEM((B, D), BF16), pltpu.VMEM((B, D), BF16), pltpu.VMEM((B, D), F32),
                dma((2, 2, H)), dma((2, 3, H)), dma((2, 3, H)), dma((2, H)),
                dma((2, 4)), dma((2, 4)), dma((4,)), dma((4,)),
                dma((3, H)), dma((3, H)), dma((2, H)), dma((2, H)), dma((2,)), dma((2,)),
                dma((4,)),
            ],
            compiler_params=pltpu.CompilerParams(
                collective_id=0, has_side_effects=True, vmem_limit_bytes=60 * 2**20),
            name="mlp_backward",
        )(x, dy, gate, up, w_gate, w_up, w_down)
        base, base_last, dwg, dwu, dwd, early, last = out[:7]
        last = lax.ppermute(last, "tp", [(2, 0), (3, 1), (4, 6), (5, 7)])
        dx, *grads = finish(S, base, early, dwg, dwu, dwd)
        last = (base_last + last.astype(F32)).astype(BF16)
        return lax.dynamic_update_slice(dx, last, (S - L, 0)), *grads

    both = P(("dp", "tp"), None)
    cols = P("dp", "tp")
    return jax.shard_map(
        step, mesh=mesh,
        in_specs=(both, both, cols, cols, P(None, "tp"), P(None, "tp"), P("tp", None)),
        out_specs=(both, cols, cols, both), check_vma=False)
```
